16 devices in a mesh: dp: 4 (over z, y), tp: 4 (over x, core).
Axes of the slice: x: 2, y: 2, z: 2, core: 2. Of those that a mesh axis runs over, the one named last changes fastest.
Arguments:
- x: bfloat16 [8, 192, 2560], P('dp', 'tp'), parts along dimension 0
- start: int32 [8], P('dp'), parts along dimension 0
- k_local: bfloat16 [8, 1024, 4, 256], P('dp', None, 'tp'), parts along dimension 0
- v_local: bfloat16 [8, 1024, 4, 256], P('dp', None, 'tp'), parts along dimension 0
- k_global: bfloat16 [8, 12480, 4, 256], P('dp', None, 'tp'), parts along dimension 0
- v_global: bfloat16 [8, 12480, 4, 256], P('dp', None, 'tp'), parts along dimension 0
- norms: float32 [2, 4, 2560], replicated
- w_q: bfloat16 [2, 2560, 2048], P(None, None, 'tp')
- w_k: bfloat16 [2, 2560, 1024], P(None, None, 'tp')
- w_v: bfloat16 [2, 2560, 1024], P(None, None, 'tp')
- w_o: bfloat16 [2, 2048, 2560], P(None, 'tp')
- w_gate: bfloat16 [2, 2560, 10240], P(None, None, 'tp')
- w_up: bfloat16 [2, 2560, 10240], P(None, None, 'tp')
- w_down: bfloat16 [2, 10240, 2560], P(None, 'tp')
Outputs:
- output 1: bfloat16 [8, 192, 2560], P('dp', 'tp'), parts along dimension 0
- output 2: bfloat16 [8, 1024, 4, 256], P('dp', None, 'tp'), parts along dimension 0
- output 3: bfloat16 [8, 1024, 4, 256], P('dp', None, 'tp'), parts along dimension 0
- output 4: bfloat16 [8, 12480, 4, 256], P('dp', None, 'tp'), parts along dimension 0
- output 5: bfloat16 [8, 12480, 4, 256], P('dp', None, 'tp'), parts along dimension 0
There are 4 independent parts. The reference program is written for one: setup_inputs(seed, part) draws one part's arguments, and reference() takes and returns one part's arrays. A program takes and returns all parts, laid end to end along the dimension named above; an argument that names none is the same for every part.
All inputs are finite; a program needn't handle non-finite values.
Results may differ from the reference program's by a relative error of at most 0.02.
Values are sent between devices in bfloat16 or wider.
A program may use at most 1 GiB of HBM per device.

```python
import jax
import jax.numpy as jnp
from jax import lax

BATCH_SEQS = 2
CHUNK_LEN = 192
PAST_MAX = 12288
D_MODEL = 2560
NUM_HEADS = 8
NUM_KV_HEADS = 4
HEAD_DIM = 256
FFN_DIM = 10240
WINDOW_LEN = 1024

CACHE_LEN = PAST_MAX + CHUNK_LEN
QUERY_BLOCK = min(CHUNK_LEN, 64)
QUERY_SCALE = HEAD_DIM ** -0.5
SOFT_CAP = 50.0
NORM_EPS = 1e-6
ROPE_BASE = 10000.0


def setup_inputs(seed: int = 0, part: int = 0) -> dict:
    part_keys = jax.random.split(jax.random.fold_in(jax.random.key(seed), part), 8)
    shared_keys = jax.random.split(jax.random.key(seed + 1), 9)
    q_width = NUM_HEADS * HEAD_DIM
    kv_width = NUM_KV_HEADS * HEAD_DIM
    local_shape = (BATCH_SEQS, WINDOW_LEN, NUM_KV_HEADS, HEAD_DIM)
    global_shape = (BATCH_SEQS, CACHE_LEN, NUM_KV_HEADS, HEAD_DIM)
    start_draw = jax.random.randint(part_keys[1], (BATCH_SEQS,), PAST_MAX // 2, PAST_MAX + 1, dtype=jnp.int32)
    top_seq = jax.random.randint(part_keys[2], (), 0, BATCH_SEQS, dtype=jnp.int32)
    start = jnp.where(jnp.arange(BATCH_SEQS, dtype=jnp.int32) == top_seq, PAST_MAX, start_draw).astype(jnp.int32)
    return {
        'x': jax.random.normal(part_keys[0], (BATCH_SEQS, CHUNK_LEN, D_MODEL), jnp.float32).astype(jnp.bfloat16),
        'start': start,
        'k_local': jax.random.normal(part_keys[3], local_shape, jnp.float32).astype(jnp.bfloat16),
        'v_local': jax.random.normal(part_keys[4], local_shape, jnp.float32).astype(jnp.bfloat16),
        'k_global': jax.random.normal(part_keys[5], global_shape, jnp.float32).astype(jnp.bfloat16),
        'v_global': jax.random.normal(part_keys[6], global_shape, jnp.float32).astype(jnp.bfloat16),
        'norms': 0.25 * jax.random.normal(shared_keys[0], (2, 4, D_MODEL), jnp.float32),
        'w_q': (jax.random.normal(shared_keys[1], (2, D_MODEL, q_width), jnp.float32) * D_MODEL ** -0.5).astype(jnp.bfloat16),
        'w_k': (jax.random.normal(shared_keys[2], (2, D_MODEL, kv_width), jnp.float32) * D_MODEL ** -0.5).astype(jnp.bfloat16),
        'w_v': (jax.random.normal(shared_keys[3], (2, D_MODEL, kv_width), jnp.float32) * D_MODEL ** -0.5).astype(jnp.bfloat16),
        'w_o': (jax.random.normal(shared_keys[4], (2, q_width, D_MODEL), jnp.float32) * q_width ** -0.5).astype(jnp.bfloat16),
        'w_gate': (jax.random.normal(shared_keys[5], (2, D_MODEL, FFN_DIM), jnp.float32) * D_MODEL ** -0.5).astype(jnp.bfloat16),
        'w_up': (jax.random.normal(shared_keys[6], (2, D_MODEL, FFN_DIM), jnp.float32) * D_MODEL ** -0.5).astype(jnp.bfloat16),
        'w_down': (jax.random.normal(shared_keys[7], (2, FFN_DIM, D_MODEL), jnp.float32) * FFN_DIM ** -0.5).astype(jnp.bfloat16),
    }


def rms_norm(hidden, scale):
    hidden_f32 = hidden.astype(jnp.float32)
    inv_rms = lax.rsqrt(jnp.mean(hidden_f32 * hidden_f32, axis=-1, keepdims=True) + NORM_EPS)
    return hidden_f32 * inv_rms * (1.0 + scale)


def rope_apply(projected, positions):
    half_dim = projected.shape[-1] // 2
    inv_freq = ROPE_BASE ** (jnp.arange(half_dim, dtype=jnp.float32) * (-2.0 / projected.shape[-1]))
    angles = positions.astype(jnp.float32)[..., None] * inv_freq
    cos_tab = jnp.cos(angles)[..., None, :]
    sin_tab = jnp.sin(angles)[..., None, :]
    lead_half = projected[..., :half_dim]
    tail_half = projected[..., half_dim:]
    return jnp.concatenate([lead_half * cos_tab - tail_half * sin_tab, tail_half * cos_tab + lead_half * sin_tab], axis=-1)


def window_positions(start, window):
    slot_ids = jnp.arange(window, dtype=jnp.int32)
    last_pos = start[:, None] - 1
    return last_pos - jnp.remainder(last_pos - slot_ids[None, :], window)


def window_write(cache, fresh, start):
    window = cache.shape[1]
    chunk_len = fresh.shape[1]
    keep_len = min(chunk_len, window)
    tail_rows = jnp.pad(fresh[:, chunk_len - keep_len:], ((0, 0), (0, window - keep_len), (0, 0), (0, 0)))
    first_pos = start + (chunk_len - keep_len)
    rolled = jax.vmap(lambda rows, amount: jnp.roll(rows, amount, axis=0))(tail_rows, jnp.remainder(first_pos, window))
    slot_ids = jnp.arange(window, dtype=jnp.int32)
    written = jnp.remainder(slot_ids[None, :] - first_pos[:, None], window) < keep_len
    return jnp.where(written[:, :, None, None], rolled, cache)


def linear_write(cache, fresh, start):
    return jax.vmap(lambda rows, new_rows, offset: lax.dynamic_update_slice_in_dim(rows, new_rows, offset, axis=0))(cache, fresh, start)


def attend_seq(q_seq, k_seq, v_seq, q_pos, k_pos, window):
    chunk_len, heads, head_dim = q_seq.shape
    kv_heads = k_seq.shape[1]
    keys_f32 = k_seq.astype(jnp.float32)
    vals_f32 = v_seq.astype(jnp.float32)
    q_blocks = q_seq.reshape(chunk_len // QUERY_BLOCK, QUERY_BLOCK, kv_heads, heads // kv_heads, head_dim)
    pos_blocks = q_pos.reshape(chunk_len // QUERY_BLOCK, QUERY_BLOCK)

    def one_block(item):
        q_blk, p_blk = item
        scores = jnp.einsum('qkgd,tkd->kgqt', q_blk.astype(jnp.float32), keys_f32) * QUERY_SCALE
        capped = SOFT_CAP * jnp.tanh(scores / SOFT_CAP)
        allowed = k_pos[None, :] <= p_blk[:, None]
        if window > 0:
            allowed = allowed & (k_pos[None, :] > p_blk[:, None] - window) & (k_pos[None, :] >= 0)
        masked = jnp.where(allowed, capped, -1e30)
        weights = jnp.exp(masked - jnp.max(masked, axis=-1, keepdims=True))
        probs = (weights / jnp.sum(weights, axis=-1, keepdims=True)).astype(jnp.bfloat16)
        block_out = jnp.einsum('kgqt,tkd->qkgd', probs.astype(jnp.float32), vals_f32)
        return block_out.astype(jnp.bfloat16)

    all_blocks = lax.map(one_block, (q_blocks, pos_blocks))
    return all_blocks.reshape(chunk_len, heads * head_dim)


def attention_half(hidden, start, k_cache, v_cache, norm_pre, norm_post, w_q, w_k, w_v, w_o, is_local):
    num_seqs = hidden.shape[0]
    positions = start[:, None] + jnp.arange(CHUNK_LEN, dtype=jnp.int32)[None, :]
    flat = rms_norm(hidden, norm_pre).astype(jnp.bfloat16).reshape(num_seqs * CHUNK_LEN, D_MODEL)
    q_proj = jnp.dot(flat, w_q, preferred_element_type=jnp.float32).reshape(num_seqs, CHUNK_LEN, NUM_HEADS, HEAD_DIM)
    k_proj = jnp.dot(flat, w_k, preferred_element_type=jnp.float32).reshape(num_seqs, CHUNK_LEN, NUM_KV_HEADS, HEAD_DIM)
    v_proj = jnp.dot(flat, w_v, preferred_element_type=jnp.float32).reshape(num_seqs, CHUNK_LEN, NUM_KV_HEADS, HEAD_DIM)
    q_rot = rope_apply(q_proj, positions).astype(jnp.bfloat16)
    k_new = rope_apply(k_proj, positions).astype(jnp.bfloat16)
    v_new = v_proj.astype(jnp.bfloat16)
    k_old = k_cache.astype(k_new.dtype)
    v_old = v_cache.astype(v_new.dtype)
    if is_local:
        window = WINDOW_LEN
        k_keys = jnp.concatenate([k_old, k_new], axis=1)
        v_keys = jnp.concatenate([v_old, v_new], axis=1)
        key_pos = jnp.concatenate([window_positions(start, WINDOW_LEN), positions], axis=1)
        k_next = window_write(k_old, k_new, start)
        v_next = window_write(v_old, v_new, start)
    else:
        window = 0
        k_next = linear_write(k_old, k_new, start)
        v_next = linear_write(v_old, v_new, start)
        k_keys = k_next
        v_keys = v_next
        key_pos = jnp.broadcast_to(jnp.arange(CACHE_LEN, dtype=jnp.int32)[None, :], (num_seqs, CACHE_LEN))
    mixed = lax.map(lambda item: attend_seq(item[0], item[1], item[2], item[3], item[4], window), (q_rot, k_keys, v_keys, positions, key_pos))
    attn_out = jnp.dot(mixed.reshape(num_seqs * CHUNK_LEN, NUM_HEADS * HEAD_DIM), w_o, preferred_element_type=jnp.float32).astype(jnp.bfloat16)
    attn_out = attn_out.reshape(num_seqs, CHUNK_LEN, D_MODEL)
    x_next = (hidden.astype(jnp.float32) + rms_norm(attn_out, norm_post)).astype(jnp.bfloat16)
    return x_next, k_next, v_next


def mlp_half(hidden, norm_pre, norm_post, w_gate, w_up, w_down):
    num_seqs = hidden.shape[0]
    flat = rms_norm(hidden, norm_pre).astype(jnp.bfloat16).reshape(num_seqs * CHUNK_LEN, D_MODEL)
    gate_proj = jnp.dot(flat, w_gate, preferred_element_type=jnp.float32)
    up_proj = jnp.dot(flat, w_up, preferred_element_type=jnp.float32)
    gated = (jax.nn.gelu(gate_proj, approximate=True) * up_proj).astype(jnp.bfloat16)
    down_out = jnp.dot(gated, w_down, preferred_element_type=jnp.float32).astype(jnp.bfloat16).reshape(num_seqs, CHUNK_LEN, D_MODEL)
    return (hidden.astype(jnp.float32) + rms_norm(down_out, norm_post)).astype(jnp.bfloat16)


def reference(x, start, k_local, v_local, k_global, v_global, norms, w_q, w_k, w_v, w_o, w_gate, w_up, w_down):
    hidden, k_local_new, v_local_new = attention_half(x, start, k_local, v_local, norms[0, 0], norms[0, 1], w_q[0], w_k[0], w_v[0], w_o[0], True)
    hidden = mlp_half(hidden, norms[0, 2], norms[0, 3], w_gate[0], w_up[0], w_down[0])
    hidden, k_global_new, v_global_new = attention_half(hidden, start, k_global, v_global, norms[1, 0], norms[1, 1], w_q[1], w_k[1], w_v[1], w_o[1], False)
    hidden = mlp_half(hidden, norms[1, 2], norms[1, 3], w_gate[1], w_up[1], w_down[1])
    return (hidden, k_local_new, v_local_new, k_global_new, v_global_new)
```

```python
import functools

import jax
import jax.numpy as jnp
import numpy as np
from jax import lax
from jax.experimental import pallas as pl
from jax.experimental.pallas import tpu as pltpu
from jax.sharding import PartitionSpec as P

BF = jnp.bfloat16
F32 = jnp.float32
MESH = pl.DeviceIdType.MESH
NORM_EPS = 1e-6
ROPE_BASE = 10000.0
LOG2E = 1.4426950408889634
S_IN = 1.0 / (50.0 * 16.0)
S_OUT = 50.0 * LOG2E
S_OFF = 36.0 * LOG2E

D = 2560
HALF = 1280
TOK = 192
BLK = 48
HD = 256
WIN = 1024
VMEM_LIMIT = 67000000
TWO = 2
PAIR = range(TWO)


def dot(a, b):
    return jnp.dot(a, b, preferred_element_type=F32)


def dot_t(a, b):
    return lax.dot_general(a, b, (((1,), (1,)), ((), ())), preferred_element_type=F32)


def soft_weights(scores):
    return jnp.exp2(jnp.tanh(scores * S_IN) * S_OUT - S_OFF)


def rope_into(proj, cos, sin, q_dst, k_dst):
    for head, (ref, row) in enumerate(((q_dst, 0), (q_dst, TOK), (k_dst, 0))):
        lead = proj[:, head * HD:head * HD + 128]
        tail = proj[:, head * HD + 128:(head + 1) * HD]
        ref[row:row + TOK, :128] = (lead * cos - tail * sin).astype(BF)
        ref[row:row + TOK, 128:] = (tail * cos + lead * sin).astype(BF)


class Peers:
    def __init__(self):
        dp = lax.axis_index("dp")
        tp = lax.axis_index("tp")
        self.x = tp // 2
        self.c = lax.rem(tp, 2)
        self.mate = (dp, tp + 1 - 2 * self.c)
        self.far = (dp, lax.rem(tp + 2, 4))

    def barrier(self):
        sem = pltpu.get_barrier_semaphore()
        for peer in (self.mate, self.far):
            pl.semaphore_signal(sem, inc=1, device_id=peer, device_id_type=MESH)
        pl.semaphore_wait(sem, 2)


def remote(src, dst, send, recv, peer):
    return pltpu.make_async_remote_copy(src_ref=src, dst_ref=dst, send_sem=send, recv_sem=recv, device_id=peer, device_id_type=MESH)


def norm_rows(act, h, w):
    def body(i, _):
        xb, cb, r = i // 6, (i // 3) % 2, pl.multiple_of((i % 3) * 16, 16)
        rows = act[h, xb, cb, pl.ds(r, 16), :].astype(F32)
        inv = lax.rsqrt(jnp.sum(rows * rows, axis=-1, keepdims=True) * (1.0 / D) + NORM_EPS)
        act[h, xb, cb, pl.ds(r, 16), :] = (rows * inv * w).astype(BF)
        return 0
    lax.fori_loop(0, 12, body, 0)


class Exchange:
    def __init__(self, peers, pbuf, ds, dr, es, er, d_sem, e_sem):
        self.p, self.pbuf, self.ds, self.dr, self.es, self.er = peers, pbuf, ds, dr, es, er
        self.d_sem, self.e_sem = d_sem, e_sem

    def d_copy(self, h, n):
        return remote(self.ds.at[h, n], self.dr.at[h, n], self.d_sem.at[0, h, n], self.d_sem.at[1, h, n], self.p.mate)

    def e_copy(self, h, n):
        return remote(self.es.at[h, n], self.er.at[h, n], self.e_sem.at[0, h, n], self.e_sem.at[1, h, n], self.p.far)

    def give(self, h, n, part):
        self.pbuf[n] = part.reshape(2, 2, BLK, HALF)
        self.ds[h, n] = self.pbuf[n, :, 1 - self.p.c].astype(BF)
        self.d_copy(h, n).start()

    def send(self, h, n):
        copy = self.d_copy(h, n)
        copy.wait_recv()
        self.es[h, n] = (self.pbuf[n, :, self.p.c] + self.dr[h, n].astype(F32)).astype(BF)
        self.e_copy(h, n).start()
        copy.wait_send()

    def take(self, h, xres, w_post, act, w_pre):
        for n in PAIR:
            self.e_copy(h, n).wait()
        c = self.p.c

        def body(i, _):
            xb, r = i // 3, pl.ds(pl.multiple_of((i % 3) * 16, 16), 16)
            ys = [(self.es[h, n, xb, r, :].astype(F32) + self.er[h, n, xb, r, :].astype(F32)).astype(BF).astype(F32) for n in PAIR]
            inv = lax.rsqrt(sum(jnp.sum(y * y, axis=-1, keepdims=True) for y in ys) * (1.0 / D) + NORM_EPS)
            news = []
            for n in PAIR:
                cols = slice(n * HALF, (n + 1) * HALF)
                new = (xres[h, xb, r, cols].astype(F32) + ys[n] * inv * w_post[:, cols]).astype(BF)
                xres[h, xb, r, cols] = new
                news.append(new.astype(F32))
            inv = lax.rsqrt(sum(jnp.sum(v * v, axis=-1, keepdims=True) for v in news) * (1.0 / D) + NORM_EPS)
            for n in PAIR:
                cols = slice(n * HALF, (n + 1) * HALF)
                act[h, xb, c, r, cols] = (news[n] * inv * w_pre[:, cols]).astype(BF)
            return 0
        lax.fori_loop(0, 6, body, 0)


class Final:
    def __init__(self, peers, pbuf, ds, dr, es, er, d_sem, e_sem):
        self.p, self.pbuf, self.ds, self.dr, self.es, self.er = peers, pbuf, ds, dr, es, er
        self.d_sem, self.e_sem = d_sem, e_sem

    d_copy = Exchange.d_copy
    give = Exchange.give

    def e_copy(self, h, n):
        return remote(self.es.at[h, n, 1 - self.p.x], self.er.at[h, n], self.e_sem.at[0, h, n], self.e_sem.at[1, h, n], self.p.far)

    send = Exchange.send

    def take(self, h, xres, w_post, out):
        for n in PAIR:
            self.e_copy(h, n).wait()
        x = self.p.x

        def body(i, _):
            r = pl.ds(pl.multiple_of(i * 16, 16), 16)
            ys = [(self.es[h, n, x, r, :].astype(F32) + self.er[h, n, r, :].astype(F32)).astype(BF).astype(F32) for n in PAIR]
            inv = lax.rsqrt(sum(jnp.sum(y * y, axis=-1, keepdims=True) for y in ys) * (1.0 / D) + NORM_EPS)
            for n in PAIR:
                cols = slice(n * HALF, (n + 1) * HALF)
                out[h, r, cols] = (xres[h, x, r, cols].astype(F32) + ys[n] * inv * w_post[:, cols]).astype(BF)
            return 0
        lax.fori_loop(0, 3, body, 0)


class Shared:
    def __init__(self, peers, act, sem):
        self.p, self.act, self.sem = peers, act, sem

    def copy(self, h):
        view = self.act.at[h, :, self.p.c]
        return remote(view, view, self.sem.at[0, h], self.sem.at[1, h], self.p.mate)


def load(src, dst, sem):
    copy = pltpu.make_async_copy(src, dst, sem)
    copy.start()
    return copy


def load_mlp(layer, w, buf, sems):
    return [load(w.at[layer, :, pl.ds(n * HALF, HALF)], buf.at[n], sems.at[n]) for n in PAIR]


def gate_up(act, h, wg, wu, hid):
    def body(n, _):
        g = act[h].reshape(TOK, D)
        gate = dot(g, wg[n])
        up = dot(g, wu[n])
        hid[n] = (jax.nn.gelu(gate, approximate=True) * up).astype(BF)
        return 0
    lax.fori_loop(0, 2, body, 0)


def down(hid, wd, n):
    return dot(hid[0], wd[n, :HALF]) + dot(hid[1], wd[n, HALF:])


def first_kernel(start, invf, norms, x_in, kl, vl, wq, wk, wv, wo, wg, wu, wd,
                 q1_out, k1_out, v1_out, xres_out, k0_out, v0_out,
                 act, xres, kc, vc, qs, ks, vs, obuf, hid, pbuf, ds, dr, es, er, wgb, wub, wdb, cosb, sinb, q1s,
                 ag_sem, d_sem, e_sem, g_sem, w_sem, o_sem):
    p = Peers()
    loads = [load(wq.at[0], wdb.at[0, :, pl.ds(0, 512)], w_sem.at[0]),
             load(wk.at[0], wdb.at[0, :, pl.ds(512, 256)], w_sem.at[1]),
             load(wv.at[0], wdb.at[0, :, pl.ds(768, 256)], w_sem.at[2]),
             load(kl, kc, w_sem.at[3]),
             load(vl, vc, w_sem.at[4])]
    load_o = [load(wo.at[0, :, pl.ds(n * HALF, HALF)], wdb.at[1, pl.ds(n * 512, 512), :], w_sem.at[5 + n]) for n in PAIR]
    own = [load(x_in.at[h], act.at[h, p.x, p.c], w_sem.at[7 + h]) for h in PAIR]
    p.barrier()

    def ag_mate(h):
        return remote(x_in.at[h], act.at[h, p.x, p.c], ag_sem.at[0, 0, h], ag_sem.at[0, 1, h], p.mate)

    def ag_far(h):
        return remote(x_in.at[h], act.at[h, p.x, p.c], ag_sem.at[1, 0, h], ag_sem.at[1, 1, h], p.far)

    def ag_pass(h):
        view = act.at[h, 1 - p.x, p.c]
        return remote(view, view, ag_sem.at[2, 0, h], ag_sem.at[2, 1, h], p.mate)

    for h in PAIR:
        ag_far(h).start()
        ag_mate(h).start()
    load_g = load_mlp(0, wg, wgb, w_sem.at[pl.ds(9, 2)])
    load_u = load_mlp(0, wu, wub, w_sem.at[pl.ds(11, 2)])

    for h in PAIR:
        pos = (lax.broadcasted_iota(jnp.int32, (TOK, 128), 0) + start[h]).astype(F32)
        angle = pos * invf[...]
        cosb[h] = jnp.cos(angle)
        sinb[h] = jnp.sin(angle)

    w0 = 1.0 + norms[0]
    w1 = 1.0 + norms[1]

    def ag_arrive(h):
        ag_far(h).wait_recv()
        ag_pass(h).start()

    def ag_finish(h):
        own[h].wait()
        ag_mate(h).wait_recv()
        ag_pass(h).wait()
        ag_mate(h).wait_send()
        ag_far(h).wait_send()
        xres[h] = act[h, :, p.c]
        norm_rows(act, h, w0[0:1])

    def local_attention(h):
        q = qs[...]
        row = lax.broadcasted_iota(jnp.int32, (2 * TOK, 1), 0)
        i = jnp.where(row >= TOK, row - TOK, row)
        least = jnp.maximum(i + 1, WIN - start[h])
        acc = jnp.zeros((2 * TOK, HD), F32)
        total = jnp.zeros((2 * TOK, 1), F32)
        for b in PAIR:
            slot = lax.broadcasted_iota(jnp.int32, (1, 512), 1) + b * 512
            age = jnp.bitwise_and(slot - start[h], WIN - 1)
            wts = jnp.where(age >= least, soft_weights(dot_t(q, kc[h, b * 512:(b + 1) * 512, :])), 0.0)
            total += jnp.sum(wts, axis=-1, keepdims=True)
            acc += dot(wts.astype(BF), vc[h, b * 512:(b + 1) * 512, :])
        key = lax.broadcasted_iota(jnp.int32, (1, TOK), 1)
        wts = jnp.where(key <= i, soft_weights(dot_t(q, ks[h])), 0.0)
        total += jnp.sum(wts, axis=-1, keepdims=True)
        acc += dot(wts.astype(BF), vs[h])
        o = (acc / total).astype(BF)
        obuf[:, :HD] = o[:TOK]
        obuf[:, HD:] = o[TOK:]

    ex = [Exchange(p, pbuf, ds, dr, es, er.at[s], d_sem.at[s], e_sem.at[s]) for s in PAIR]
    sh = [Shared(p, act, g_sem.at[s]) for s in PAIR]

    for h in PAIR:
        if h == 0:
            ag_arrive(0)
        ag_finish(h)
        if h == 0:
            for copy in loads:
                copy.wait()
        proj = dot(act[h].reshape(TOK, D), wdb[0, :, :1024])
        rope_into(proj, cosb[h], sinb[h], qs, ks.at[h])
        vs[h] = proj[:, 768:].astype(BF)
        local_attention(h)
        for n in PAIR:
            if h == 0:
                load_o[n].wait()
            ex[0].give(h, n, dot(obuf[...], wdb[1, n * 512:(n + 1) * 512, :]))
        if h == 0:
            ag_arrive(1)
        for n in PAIR:
            ex[0].send(h, n)
    load_d = load_mlp(0, wd, wdb, w_sem.at[pl.ds(13, 2)])
    outs = [load(ks, k0_out, o_sem.at[0]), load(vs, v0_out, o_sem.at[1])]

    def mlp(h):
        for n in PAIR:
            if h == 0:
                load_g[n].wait()
                load_u[n].wait()
        gate_up(act, h, wgb, wub, hid)
        for n in PAIR:
            if h == 0:
                load_d[n].wait()
            ex[1].give(h, n, down(hid, wdb, n))
        ex[1].send(h, 0)

    ex[0].take(0, xres, w0[1:2], act, w0[2:3])
    sh[0].copy(0).start()
    sh[0].copy(0).wait()
    mlp(0)
    ex[0].take(1, xres, w0[1:2], act, w0[2:3])
    sh[0].copy(1).start()
    ex[1].send(0, 1)
    sh[0].copy(1).wait()
    mlp(1)
    loads = [load(wq.at[1], wgb.at[0, :, pl.ds(0, 512)], w_sem.at[15]),
             load(wk.at[1], wgb.at[0, :, pl.ds(512, 256)], w_sem.at[16]),
             load(wv.at[1], wgb.at[0, :, pl.ds(768, 256)], w_sem.at[17])]
    ex[1].take(0, xres, w0[3:4], act, w1[0:1])
    sh[1].copy(0).start()
    ex[1].send(1, 1)
    for copy in outs:
        copy.wait()
    for h in PAIR:
        if h == 1:
            ex[1].take(1, xres, w0[3:4], act, w1[0:1])
            sh[1].copy(1).start()
            outs = [load(xres, xres_out, o_sem.at[2])]
        sh[1].copy(h).wait()
        if h == 0:
            for copy in loads:
                copy.wait()
        proj = dot(act[h].reshape(TOK, D), wgb[0, :, :1024])
        rope_into(proj, cosb[h], sinb[h], q1s.at[h], ks.at[h])
        vs[h] = proj[:, 768:].astype(BF)
    outs += [load(q1s, q1_out, o_sem.at[3]), load(ks, k1_out, o_sem.at[4]), load(vs, v1_out, o_sem.at[5])]
    for copy in outs:
        copy.wait()


def last_kernel(norms, o_in, x_in, wo, wg, wu, wd, out_ref,
                act, xres, obuf, hid, pbuf, ds, dr, es, er, fr, wob, wgb, wub, wdb,
                d_sem, e_sem, g_sem, w_sem):
    p = Peers()
    load_in = [load(o_in, obuf, w_sem.at[0]), load(x_in, xres, w_sem.at[1])]
    load_o = [load(wo.at[1, :, pl.ds(n * HALF, HALF)], wob.at[n], w_sem.at[2 + n]) for n in PAIR]
    load_g = load_mlp(1, wg, wgb, w_sem.at[pl.ds(4, 2)])
    load_u = load_mlp(1, wu, wub, w_sem.at[pl.ds(6, 2)])
    load_d = load_mlp(1, wd, wdb, w_sem.at[pl.ds(8, 2)])
    p.barrier()
    w1 = 1.0 + norms[1]
    first = Exchange(p, pbuf, ds, dr, es, er, d_sem.at[0], e_sem.at[0])
    final = Final(p, pbuf, ds, dr, es, fr, d_sem.at[1], e_sem.at[1])
    sh = Shared(p, act, g_sem)
    for copy in load_in:
        copy.wait()
    for h in PAIR:
        for n in PAIR:
            if h == 0:
                load_o[n].wait()
            first.give(h, n, dot(obuf[h], wob[n]))
        for n in PAIR:
            first.send(h, n)

    def mlp(h):
        for n in PAIR:
            if h == 0:
                load_g[n].wait()
                load_u[n].wait()
        gate_up(act, h, wgb, wub, hid)
        for n in PAIR:
            if h == 0:
                load_d[n].wait()
            final.give(h, n, down(hid, wdb, n))
        final.send(h, 0)

    first.take(0, xres, w1[1:2], act, w1[2:3])
    sh.copy(0).start()
    sh.copy(0).wait()
    mlp(0)
    first.take(1, xres, w1[1:2], act, w1[2:3])
    sh.copy(1).start()
    final.send(0, 1)
    sh.copy(1).wait()
    mlp(1)
    final.send(1, 1)
    final.take(0, xres, w1[3:4], out_ref)
    final.take(1, xres, w1[3:4], out_ref)


def shifted(ref, off, n):
    base = pl.multiple_of((off // 8) * 8, 8)
    rows = ref[pl.ds(base, n + 8), :]
    return pltpu.roll(rows, lax.rem(n + 8 - (off - base), n + 8), 0)[:n]


TILE = 1024
PAST = 12288
CACHE = PAST + TOK
NT = PAST // TILE
WROWS = TOK + 16


def global_kernel(start, q_in, k_new, v_new, k0_new, v0_new, kl, vl, kg, vg,
                  o_out, kl_out, vl_out, kg_out, vg_out,
                  kb, vb, kt, vt, kwin, vwin, lbuf, ext, pb, acc, tot, obuf, in_sem, out_sem, t_sem, w_sem, l_sem):
    caches = ((kg, kb, kg_out, kt, kwin, k_new), (vg, vb, vg_out, vt, vwin, v_new))

    def tile_in(a, h, t):
        src, buf = caches[a][0], caches[a][1]
        return pltpu.make_async_copy(src.at[h, pl.ds(pl.multiple_of(t * TILE, TILE), TILE)], buf.at[h, t], in_sem.at[a, h, t])

    def tile_out(a, h, t):
        buf, dst = caches[a][1], caches[a][2]
        return pltpu.make_async_copy(buf.at[h, t], dst.at[h, pl.ds(pl.multiple_of(t * TILE, TILE), TILE)], out_sem.at[a, h, t])

    def tail_in(a, h):
        return pltpu.make_async_copy(caches[a][0].at[h, pl.ds(PAST, TOK)], caches[a][3].at[h], t_sem.at[0, a, h])

    def tail_out(a, h):
        return pltpu.make_async_copy(caches[a][3].at[h], caches[a][2].at[h, pl.ds(PAST, TOK)], t_sem.at[1, a, h])

    def win_at(h):
        s = start[h]
        return pl.multiple_of(jnp.minimum((s // 16) * 16, CACHE - WROWS), 16)

    def win_in(a, h):
        return pltpu.make_async_copy(caches[a][0].at[h, pl.ds(win_at(h), WROWS)], caches[a][4].at[h], w_sem.at[0, a, h])

    def win_out(a, h):
        return pltpu.make_async_copy(caches[a][4].at[h], caches[a][2].at[h, pl.ds(win_at(h), WROWS)], w_sem.at[1, a, h])

    local = ((kl, k0_new, kl_out), (vl, v0_new, vl_out))
    for a in PAIR:
        pltpu.make_async_copy(local[a][0], lbuf.at[a], l_sem.at[a]).start()
    for h in PAIR:
        for t in range(NT):
            for a in PAIR:
                tile_in(a, h, t).start()
        for a in PAIR:
            win_in(a, h).start()
            tail_in(a, h).start()

    for a in PAIR:
        pltpu.make_async_copy(local[a][0], lbuf.at[a], l_sem.at[a]).wait()
        for h in PAIR:
            fresh = local[a][1][h].astype(F32)
            ext[0:TOK] = fresh
            ext[WIN:WIN + TOK] = fresh
            off = jnp.bitwise_and(-start[h], WIN - 1)
            for b in range(4):
                rows = shifted(ext, off + b * 256, 256)
                age = jnp.bitwise_and(lax.broadcasted_iota(jnp.int32, (256, 1), 0) + (b * 256) + off, WIN - 1)
                old = lbuf[a, h, b * 256:(b + 1) * 256, :].astype(F32)
                lbuf[a, h, b * 256:(b + 1) * 256, :] = jnp.where(age < TOK, rows, old).astype(BF)
        pltpu.make_async_copy(lbuf.at[a], local[a][2], l_sem.at[a]).start()

    row = lax.broadcasted_iota(jnp.int32, (2 * TOK, 1), 0)
    qi = jnp.where(row >= TOK, row - TOK, row)

    for h in PAIR:
        acc[...] = jnp.zeros_like(acc)
        tot[...] = jnp.zeros_like(tot)
        q = q_in[h]

        def fetch(t):
            for a in PAIR:
                tile_in(a, h, t).wait()
                tile_out(a, h, t).start()

        def weigh(t, b, masked):
            wts = soft_weights(dot_t(q, kb[h, t, b * 256:(b + 1) * 256, :]))
            if masked:
                slot = lax.broadcasted_iota(jnp.int32, (1, 256), 1) + (t * TILE + b * 256)
                wts = jnp.where(slot < start[h], wts, 0.0)
            tot[...] += wts[:, :128] + wts[:, 128:]
            pb[:, b * 256:(b + 1) * 256] = wts.astype(BF)

        def tile(t, masked):
            fetch(t)
            for b in range(TILE // 256):
                weigh(t, b, masked)
            acc[...] += dot(pb[...], vb[h, t])

        full = start[h] // TILE

        def full_tile(t, _):
            tile(t, False)
            return 0

        lax.fori_loop(0, full, full_tile, 0)

        @pl.when(lax.rem(start[h], TILE) != 0)
        def _():
            tile(full, True)

        def rest(t, _):
            fetch(t)
            return 0

        lax.fori_loop((start[h] + TILE - 1) // TILE, NT, rest, 0)
        wts = jnp.where(lax.broadcasted_iota(jnp.int32, (1, TOK), 1) <= qi, soft_weights(dot_t(q, k_new[h])), 0.0)
        total = jnp.sum(tot[...], axis=-1, keepdims=True) + jnp.sum(wts, axis=-1, keepdims=True)
        o = ((acc[...] + dot(wts.astype(BF), v_new[h])) / total).astype(BF)
        obuf[h, :, :HD] = o[:TOK]
        obuf[h, :, HD:] = o[TOK:]

        for a in PAIR:
            tail_in(a, h).wait()
            tail_out(a, h).start()
            win_in(a, h).wait()
            ext[16:16 + TOK] = caches[a][5][h].astype(F32)
            shift = win_at(h) - start[h]
            rows = shifted(ext, shift + 16, WROWS)
            idx = lax.broadcasted_iota(jnp.int32, (WROWS, 1), 0) + shift
            win = caches[a][4]
            win[h] = jnp.where((idx >= 0) & (idx < TOK), rows, win[h].astype(F32)).astype(BF)

        def drain(t, _):
            for a in PAIR:
                tile_out(a, h, t).wait()
            return 0

        lax.fori_loop(0, NT, drain, 0)
        for a in PAIR:
            tail_out(a, h).wait()
            win_out(a, h).start()
    done = pltpu.make_async_copy(obuf, o_out, l_sem.at[2])
    done.start()
    done.wait()
    for a in PAIR:
        pltpu.make_async_copy(lbuf.at[a], local[a][2], l_sem.at[a]).wait()
        for h in PAIR:
            win_out(a, h).wait()


ANY = pl.BlockSpec(memory_space=pl.ANY)
VM = pl.BlockSpec(memory_space=pltpu.VMEM)
SM = pl.BlockSpec(memory_space=pltpu.SMEM)
DMA = pltpu.SemaphoreType.DMA


def vmem(*shape, dtype=BF):
    return pltpu.VMEM(shape, dtype)


def sds(*shape, dtype=BF):
    return jax.ShapeDtypeStruct(shape, dtype)


def run_first(start, invf, norms, x, kl, vl, *weights):
    return pl.pallas_call(
        first_kernel,
        name="first",
        out_shape=(sds(TWO, TWO * TOK, HD), sds(TWO, TOK, HD), sds(TWO, TOK, HD), sds(TWO, TWO, BLK, D), sds(TWO, TOK, HD), sds(TWO, TOK, HD)),
        in_specs=[SM, VM, VM] + [ANY] * 10,
        out_specs=(ANY,) * 6,
        scratch_shapes=[
            vmem(TWO, TWO, TWO, BLK, D), vmem(TWO, TWO, BLK, D), vmem(TWO, WIN, HD), vmem(TWO, WIN, HD), vmem(TWO * TOK, HD), vmem(TWO, TOK, HD), vmem(TWO, TOK, HD),
            vmem(TOK, 512), vmem(TWO, TOK, HALF), vmem(TWO, TWO, TWO, BLK, HALF, dtype=F32),
            vmem(TWO, TWO, TWO, BLK, HALF), vmem(TWO, TWO, TWO, BLK, HALF), vmem(TWO, TWO, TWO, BLK, HALF), vmem(TWO, TWO, TWO, TWO, BLK, HALF),
            vmem(TWO, D, HALF), vmem(TWO, D, HALF), vmem(TWO, D, HALF),
            vmem(TWO, TOK, 128, dtype=F32), vmem(TWO, TOK, 128, dtype=F32), vmem(TWO, TWO * TOK, HD),
            DMA((3, TWO, TWO)), DMA((TWO, TWO, TWO, TWO)), DMA((TWO, TWO, TWO, TWO)), DMA((TWO, TWO, TWO)), DMA((18,)), DMA((6,)),
        ],
        compiler_params=pltpu.CompilerParams(collective_id=0, has_side_effects=True, vmem_limit_bytes=VMEM_LIMIT),
    )(start, invf, norms, x, kl, vl, *weights)


def run_global(start, q, k_new, v_new, k0_new, v0_new, kl, vl, kg, vg):
    return pl.pallas_call(
        global_kernel,
        name="attend",
        out_shape=(sds(TWO, TOK, 512), sds(TWO, WIN, HD), sds(TWO, WIN, HD), sds(TWO, CACHE, HD), sds(TWO, CACHE, HD)),
        in_specs=[SM] + [VM] * 5 + [ANY] * 4,
        out_specs=(ANY,) * 5,
        scratch_shapes=[
            vmem(TWO, NT, TILE, HD), vmem(TWO, NT, TILE, HD), vmem(TWO, TOK, HD), vmem(TWO, TOK, HD), vmem(TWO, WROWS, HD), vmem(TWO, WROWS, HD),
            vmem(TWO, TWO, WIN, HD), vmem(TWO * WIN + 8, HD, dtype=F32), vmem(TWO * TOK, TILE), vmem(TWO * TOK, HD, dtype=F32),
            vmem(TWO * TOK, 128, dtype=F32), vmem(TWO, TOK, 512),
            DMA((TWO, TWO, NT)), DMA((TWO, TWO, NT)), DMA((TWO, TWO, TWO)), DMA((TWO, TWO, TWO)), DMA((3,)),
        ],
        compiler_params=pltpu.CompilerParams(has_side_effects=True, vmem_limit_bytes=VMEM_LIMIT),
    )(start, q, k_new, v_new, k0_new, v0_new, kl, vl, kg, vg)


def run_last(norms, o, x, wo, wg, wu, wd):
    return pl.pallas_call(
        last_kernel,
        name="last",
        out_shape=sds(TWO, BLK, D),
        in_specs=[VM] + [ANY] * 6,
        out_specs=VM,
        scratch_shapes=[
            vmem(TWO, TWO, TWO, BLK, D), vmem(TWO, TWO, BLK, D), vmem(TWO, TOK, 512), vmem(TWO, TOK, HALF), vmem(TWO, TWO, TWO, BLK, HALF, dtype=F32),
            vmem(TWO, TWO, TWO, BLK, HALF), vmem(TWO, TWO, TWO, BLK, HALF), vmem(TWO, TWO, TWO, BLK, HALF), vmem(TWO, TWO, TWO, BLK, HALF), vmem(TWO, TWO, BLK, HALF),
            vmem(TWO, 512, HALF), vmem(TWO, D, HALF), vmem(TWO, D, HALF), vmem(TWO, D, HALF),
            DMA((TWO, TWO, TWO, TWO)), DMA((TWO, TWO, TWO, TWO)), DMA((TWO, TWO)), DMA((10,)),
        ],
        compiler_params=pltpu.CompilerParams(collective_id=1, has_side_effects=True, vmem_limit_bytes=VMEM_LIMIT),
    )(norms, o, x, wo, wg, wu, wd)


def solution(mesh):
    act_spec = P('dp', 'tp', None)
    cache_spec = P('dp', None, 'tp', None)
    col_spec = P(None, None, 'tp')
    row_spec = P(None, 'tp', None)
    arg_specs = (act_spec, P('dp'), cache_spec, cache_spec, cache_spec, cache_spec, P(), col_spec, col_spec, col_spec, row_spec, col_spec, col_spec, row_spec)
    result_specs = (act_spec, cache_spec, cache_spec, cache_spec, cache_spec)
    inv_freq = np.power(np.float64(ROPE_BASE), np.arange(HD // 2) * (-2.0 / HD)).astype(np.float32)[None, :]

    def device_step(x, start, k_local, v_local, k_global, v_global, norms, w_q, w_k, w_v, w_o, w_gate, w_up, w_down):
        def flat(cache):
            return cache.reshape(cache.shape[0], cache.shape[1], cache.shape[3])

        kl, vl, kg, vg = flat(k_local), flat(v_local), flat(k_global), flat(v_global)
        q1, k1, v1, xres, k0, v0 = run_first(start, jnp.asarray(inv_freq), norms, x, kl, vl, w_q, w_k, w_v, w_o, w_gate, w_up, w_down)
        o1, kl_new, vl_new, kg_new, vg_new = run_global(start, q1, k1, v1, k0, v0, kl, vl, kg, vg)
        out = run_last(norms, o1, xres, w_o, w_gate, w_up, w_down)
        return (out, kl_new.reshape(k_local.shape), vl_new.reshape(v_local.shape), kg_new.reshape(k_global.shape), vg_new.reshape(v_global.shape))

    return jax.shard_map(device_step, mesh=mesh, in_specs=arg_specs, out_specs=result_specs, check_vma=False)
```

```python
import functools

import jax
import jax.numpy as jnp
import numpy as np
from jax import lax
from jax.experimental import pallas as pl
from jax.experimental.pallas import tpu as pltpu
from jax.sharding import PartitionSpec as P

BF = jnp.bfloat16
F32 = jnp.float32
MESH = pl.DeviceIdType.MESH
NORM_EPS = 1e-6
ROPE_BASE = 10000.0
LOG2E = 1.4426950408889634
S_IN = 1.0 / (50.0 * 16.0)
S_OUT = 50.0 * LOG2E
S_OFF = 36.0 * LOG2E

D = 2560
HALF = 1280
TOK = 192
BLK = 48
HD = 256
WIN = 1024
VMEM_LIMIT = 67000000
TWO = 2
PAIR = range(TWO)


def dot(a, b):
    return jnp.dot(a, b, preferred_element_type=F32)


def dot_t(a, b):
    return lax.dot_general(a, b, (((1,), (1,)), ((), ())), preferred_element_type=F32)


def soft_weights(scores):
    return jnp.exp2(jnp.tanh(scores * S_IN) * S_OUT - S_OFF)


def rope_into(proj, cos, sin, q_dst, k_dst):
    for head, (ref, row) in enumerate(((q_dst, 0), (q_dst, TOK), (k_dst, 0))):
        lead = proj[:, head * HD:head * HD + 128]
        tail = proj[:, head * HD + 128:(head + 1) * HD]
        ref[row:row + TOK, :128] = (lead * cos - tail * sin).astype(BF)
        ref[row:row + TOK, 128:] = (tail * cos + lead * sin).astype(BF)


class Peers:
    def __init__(self):
        dp = lax.axis_index("dp")
        tp = lax.axis_index("tp")
        self.x = tp // 2
        self.c = lax.rem(tp, 2)
        self.mate = (dp, tp + 1 - 2 * self.c)
        self.far = (dp, lax.rem(tp + 2, 4))

    def barrier(self):
        sem = pltpu.get_barrier_semaphore()
        for peer in (self.mate, self.far):
            pl.semaphore_signal(sem, inc=1, device_id=peer, device_id_type=MESH)
        pl.semaphore_wait(sem, 2)


def remote(src, dst, send, recv, peer):
    return pltpu.make_async_remote_copy(src_ref=src, dst_ref=dst, send_sem=send, recv_sem=recv, device_id=peer, device_id_type=MESH)


def norm_rows(act, h, w):
    def body(i, _):
        xb, cb, r = i // 6, (i // 3) % 2, pl.multiple_of((i % 3) * 16, 16)
        rows = act[h, xb, cb, pl.ds(r, 16), :].astype(F32)
        inv = lax.rsqrt(jnp.sum(rows * rows, axis=-1, keepdims=True) * (1.0 / D) + NORM_EPS)
        act[h, xb, cb, pl.ds(r, 16), :] = (rows * inv * w).astype(BF)
        return 0
    lax.fori_loop(0, 12, body, 0)


class Exchange:
    def __init__(self, peers, pbuf, ds, dr, es, er, d_sem, e_sem):
        self.p, self.pbuf, self.ds, self.dr, self.es, self.er = peers, pbuf, ds, dr, es, er
        self.d_sem, self.e_sem = d_sem, e_sem

    def d_copy(self, h, n):
        return remote(self.ds.at[h, n], self.dr.at[h, n], self.d_sem.at[0, h, n], self.d_sem.at[1, h, n], self.p.mate)

    def e_copy(self, h, n):
        return remote(self.es.at[h, n], self.er.at[h, n], self.e_sem.at[0, h, n], self.e_sem.at[1, h, n], self.p.far)

    def give(self, h, n, part):
        self.pbuf[n] = part.reshape(2, 2, BLK, HALF)
        self.ds[h, n] = self.pbuf[n, :, 1 - self.p.c].astype(BF)
        self.d_copy(h, n).start()

    def send(self, h, n):
        copy = self.d_copy(h, n)
        copy.wait_recv()
        self.es[h, n] = (self.pbuf[n, :, self.p.c] + self.dr[h, n].astype(F32)).astype(BF)
        self.e_copy(h, n).start()
        copy.wait_send()

    def take(self, h, xres, w_post, act, w_pre):
        for n in PAIR:
            self.e_copy(h, n).wait()
        c = self.p.c

        def body(i, _):
            xb, r = i // 3, pl.ds(pl.multiple_of((i % 3) * 16, 16), 16)
            ys = [(self.es[h, n, xb, r, :].astype(F32) + self.er[h, n, xb, r, :].astype(F32)).astype(BF).astype(F32) for n in PAIR]
            inv = lax.rsqrt(sum(jnp.sum(y * y, axis=-1, keepdims=True) for y in ys) * (1.0 / D) + NORM_EPS)
            news = []
            for n in PAIR:
                cols = slice(n * HALF, (n + 1) * HALF)
                new = (xres[h, xb, r, cols].astype(F32) + ys[n] * inv * w_post[:, cols]).astype(BF)
                xres[h, xb, r, cols] = new
                news.append(new.astype(F32))
            inv = lax.rsqrt(sum(jnp.sum(v * v, axis=-1, keepdims=True) for v in news) * (1.0 / D) + NORM_EPS)
            for n in PAIR:
                cols = slice(n * HALF, (n + 1) * HALF)
                act[h, xb, c, r, cols] = (news[n] * inv * w_pre[:, cols]).astype(BF)
            return 0
        lax.fori_loop(0, 6, body, 0)


class Final:
    def __init__(self, peers, pbuf, ds, dr, es, er, d_sem, e_sem):
        self.p, self.pbuf, self.ds, self.dr, self.es, self.er = peers, pbuf, ds, dr, es, er
        self.d_sem, self.e_sem = d_sem, e_sem

    d_copy = Exchange.d_copy
    give = Exchange.give

    def e_copy(self, h, n):
        return remote(self.es.at[h, n, 1 - self.p.x], self.er.at[h, n], self.e_sem.at[0, h, n], self.e_sem.at[1, h, n], self.p.far)

    send = Exchange.send

    def take(self, h, xres, w_post, out):
        for n in PAIR:
            self.e_copy(h, n).wait()
        x = self.p.x

        def body(i, _):
            r = pl.ds(pl.multiple_of(i * 16, 16), 16)
            ys = [(self.es[h, n, x, r, :].astype(F32) + self.er[h, n, r, :].astype(F32)).astype(BF).astype(F32) for n in PAIR]
            inv = lax.rsqrt(sum(jnp.sum(y * y, axis=-1, keepdims=True) for y in ys) * (1.0 / D) + NORM_EPS)
            for n in PAIR:
                cols = slice(n * HALF, (n + 1) * HALF)
                out[h, r, cols] = (xres[h, x, r, cols].astype(F32) + ys[n] * inv * w_post[:, cols]).astype(BF)
            return 0
        lax.fori_loop(0, 3, body, 0)


class Shared:
    def __init__(self, peers, act, sem):
        self.p, self.act, self.sem = peers, act, sem

    def copy(self, h):
        view = self.act.at[h, :, self.p.c]
        return remote(view, view, self.sem.at[0, h], self.sem.at[1, h], self.p.mate)


def load(src, dst, sem):
    copy = pltpu.make_async_copy(src, dst, sem)
    copy.start()
    return copy


def load_mlp(layer, w, buf, sems):
    return [load(w.at[layer, :, pl.ds(n * HALF, HALF)], buf.at[n], sems.at[n]) for n in PAIR]


def gate_up(act, h, wg, wu, hid):
    def body(n, _):
        g = act[h].reshape(TOK, D)
        gate = dot(g, wg[n])
        up = dot(g, wu[n])
        hid[n] = (jax.nn.gelu(gate, approximate=True) * up).astype(BF)
        return 0
    lax.fori_loop(0, 2, body, 0)


def down(hid, wd, n):
    return dot(hid[0], wd[n, :HALF]) + dot(hid[1], wd[n, HALF:])


def first_kernel(start, invf, norms, x_in, kl, vl, wq, wk, wv, wo, wg, wu, wd,
                 q1_out, k1_out, v1_out, xres_out, k0_out, v0_out,
                 act, xres, kc, vc, qs, ks, vs, obuf, hid, pbuf, ds, dr, es, er, wgb, wub, wdb, cosb, sinb, q1s,
                 ag_sem, d_sem, e_sem, g_sem, w_sem, o_sem):
    p = Peers()
    loads = [load(wq.at[0], wdb.at[0, :, pl.ds(0, 512)], w_sem.at[0]),
             load(wk.at[0], wdb.at[0, :, pl.ds(512, 256)], w_sem.at[1]),
             load(wv.at[0], wdb.at[0, :, pl.ds(768, 256)], w_sem.at[2]),
             load(kl, kc, w_sem.at[3]),
             load(vl, vc, w_sem.at[4])]
    load_o = [load(wo.at[0, :, pl.ds(n * HALF, HALF)], wdb.at[1, pl.ds(n * 512, 512), :], w_sem.at[5 + n]) for n in PAIR]
    own = [load(x_in.at[h], act.at[h, p.x, p.c], w_sem.at[7 + h]) for h in PAIR]
    p.barrier()

    def ag_mate(h):
        return remote(x_in.at[h], act.at[h, p.x, p.c], ag_sem.at[0, 0, h], ag_sem.at[0, 1, h], p.mate)

    def ag_far(h):
        return remote(x_in.at[h], act.at[h, p.x, p.c], ag_sem.at[1, 0, h], ag_sem.at[1, 1, h], p.far)

    def ag_pass(h):
        view = act.at[h, 1 - p.x, p.c]
        return remote(view, view, ag_sem.at[2, 0, h], ag_sem.at[2, 1, h], p.mate)

    for h in PAIR:
        ag_far(h).start()
        ag_mate(h).start()
    for h in PAIR:
        pos = (lax.broadcasted_iota(jnp.int32, (TOK, 128), 0) + start[h]).astype(F32)
        angle = pos * invf[...]
        cosb[h] = jnp.cos(angle)
        sinb[h] = jnp.sin(angle)

    w0 = 1.0 + norms[0]
    w1 = 1.0 + norms[1]

    def ag_arrive(h):
        ag_far(h).wait_recv()
        ag_pass(h).start()

    def ag_finish(h):
        own[h].wait()
        ag_mate(h).wait_recv()
        ag_pass(h).wait()
        ag_mate(h).wait_send()
        ag_far(h).wait_send()
        xres[h] = act[h, :, p.c]
        norm_rows(act, h, w0[0:1])

    def local_attention(h):
        q = qs[...]
        row = lax.broadcasted_iota(jnp.int32, (2 * TOK, 1), 0)
        i = jnp.where(row >= TOK, row - TOK, row)
        least = jnp.maximum(i + 1, WIN - start[h])
        acc = jnp.zeros((2 * TOK, HD), F32)
        total = jnp.zeros((2 * TOK, 1), F32)
        for b in PAIR:
            slot = lax.broadcasted_iota(jnp.int32, (1, 512), 1) + b * 512
            age = jnp.bitwise_and(slot - start[h], WIN - 1)
            wts = jnp.where(age >= least, soft_weights(dot_t(q, kc[h, b * 512:(b + 1) * 512, :])), 0.0)
            total += jnp.sum(wts, axis=-1, keepdims=True)
            acc += dot(wts.astype(BF), vc[h, b * 512:(b + 1) * 512, :])
        key = lax.broadcasted_iota(jnp.int32, (1, TOK), 1)
        wts = jnp.where(key <= i, soft_weights(dot_t(q, ks[h])), 0.0)
        total += jnp.sum(wts, axis=-1, keepdims=True)
        acc += dot(wts.astype(BF), vs[h])
        o = (acc / total).astype(BF)
        obuf[:, :HD] = o[:TOK]
        obuf[:, HD:] = o[TOK:]

    ex = [Exchange(p, pbuf, ds, dr, es, er.at[s], d_sem.at[s], e_sem.at[s]) for s in PAIR]
    sh = [Shared(p, act, g_sem.at[s]) for s in PAIR]

    for h in PAIR:
        if h == 0:
            ag_arrive(0)
        ag_finish(h)
        if h == 0:
            for copy in loads + load_o:
                copy.wait()
            load_g = load_mlp(0, wg, wgb, w_sem.at[pl.ds(9, 2)])
            load_u = load_mlp(0, wu, wub, w_sem.at[pl.ds(11, 2)])
        proj = dot(act[h].reshape(TOK, D), wdb[0, :, :1024])
        rope_into(proj, cosb[h], sinb[h], qs, ks.at[h])
        vs[h] = proj[:, 768:].astype(BF)
        local_attention(h)
        for n in PAIR:
            ex[0].give(h, n, dot(obuf[...], wdb[1, n * 512:(n + 1) * 512, :]))
        if h == 0:
            ag_arrive(1)
        for n in PAIR:
            ex[0].send(h, n)
    load_d = load_mlp(0, wd, wdb, w_sem.at[pl.ds(13, 2)])
    outs = [load(ks, k0_out, o_sem.at[0]), load(vs, v0_out, o_sem.at[1])]

    def mlp(h, _):
        ex[0].take(h, xres, w0[1:2], act, w0[2:3])
        sh[0].copy(h).start()

        @pl.when(h == 1)
        def _():
            ex[1].send(0, 1)

        sh[0].copy(h).wait()

        @pl.when(h == 0)
        def _():
            for copy in load_g + load_u:
                copy.wait()

        gate_up(act, h, wgb, wub, hid)

        @pl.when(h == 0)
        def _():
            for copy in load_d:
                copy.wait()

        for n in PAIR:
            ex[1].give(h, n, down(hid, wdb, n))
        ex[1].send(h, 0)
        return 0

    lax.fori_loop(0, 2, mlp, 0)
    loads = [load(wq.at[1], wgb.at[0, :, pl.ds(0, 512)], w_sem.at[15]),
             load(wk.at[1], wgb.at[0, :, pl.ds(512, 256)], w_sem.at[16]),
             load(wv.at[1], wgb.at[0, :, pl.ds(768, 256)], w_sem.at[17])]
    ex[1].take(0, xres, w0[3:4], act, w1[0:1])
    sh[1].copy(0).start()
    ex[1].send(1, 1)
    for copy in outs:
        copy.wait()
    for h in PAIR:
        if h == 1:
            ex[1].take(1, xres, w0[3:4], act, w1[0:1])
            sh[1].copy(1).start()
            outs = [load(xres, xres_out, o_sem.at[2])]
        sh[1].copy(h).wait()
        if h == 0:
            for copy in loads:
                copy.wait()
        proj = dot(act[h].reshape(TOK, D), wgb[0, :, :1024])
        rope_into(proj, cosb[h], sinb[h], q1s.at[h], ks.at[h])
        vs[h] = proj[:, 768:].astype(BF)
    outs += [load(q1s, q1_out, o_sem.at[3]), load(ks, k1_out, o_sem.at[4]), load(vs, v1_out, o_sem.at[5])]
    for copy in outs:
        copy.wait()


def last_kernel(norms, o_in, x_in, wo, wg, wu, wd, out_ref,
                act, xres, obuf, hid, pbuf, ds, dr, es, er, fr, wob, wgb, wub, wdb,
                d_sem, e_sem, g_sem, w_sem):
    p = Peers()
    load_in = [load(o_in, obuf, w_sem.at[0]), load(x_in, xres, w_sem.at[1])]
    load_o = [load(wo.at[1, :, pl.ds(n * HALF, HALF)], wob.at[n], w_sem.at[2 + n]) for n in PAIR]
    p.barrier()
    w1 = 1.0 + norms[1]
    first = Exchange(p, pbuf, ds, dr, es, er, d_sem.at[0], e_sem.at[0])
    final = Final(p, pbuf, ds, dr, es, fr, d_sem.at[1], e_sem.at[1])
    sh = Shared(p, act, g_sem)
    for copy in load_in + load_o:
        copy.wait()
    load_g = load_mlp(1, wg, wgb, w_sem.at[pl.ds(4, 2)])
    load_u = load_mlp(1, wu, wub, w_sem.at[pl.ds(6, 2)])
    load_d = load_mlp(1, wd, wdb, w_sem.at[pl.ds(8, 2)])
    for h in PAIR:
        for n in PAIR:
            first.give(h, n, dot(obuf[h], wob[n]))
        for n in PAIR:
            first.send(h, n)

    def mlp(h, _):
        first.take(h, xres, w1[1:2], act, w1[2:3])
        sh.copy(h).start()

        @pl.when(h == 1)
        def _():
            final.send(0, 1)

        sh.copy(h).wait()

        @pl.when(h == 0)
        def _():
            for copy in load_g + load_u:
                copy.wait()

        gate_up(act, h, wgb, wub, hid)

        @pl.when(h == 0)
        def _():
            for copy in load_d:
                copy.wait()

        for n in PAIR:
            final.give(h, n, down(hid, wdb, n))
        final.send(h, 0)
        return 0

    lax.fori_loop(0, 2, mlp, 0)
    final.send(1, 1)
    final.take(0, xres, w1[3:4], out_ref)
    final.take(1, xres, w1[3:4], out_ref)


def shifted(ref, off, n):
    base = pl.multiple_of((off // 8) * 8, 8)
    rows = ref[pl.ds(base, n + 8), :]
    return pltpu.roll(rows, lax.rem(n + 8 - (off - base), n + 8), 0)[:n]


TILE = 1024
PAST = 12288
CACHE = PAST + TOK
NT = PAST // TILE
WROWS = TOK + 16
AHEAD = 8
HIDE = 1e6


def global_kernel(start, q_in, k_new, v_new, k0_new, v0_new, kl, vl, kg, vg,
                  o_out, kl_out, vl_out, kg_out, vg_out,
                  kb, vb, kt, vt, kwin, vwin, lbuf, ext, pa, pb, acc, tot, obuf, in_sem, out_sem, t_sem, w_sem, l_sem):
    caches = ((kg, kb, kg_out, kt, kwin, k_new), (vg, vb, vg_out, vt, vwin, v_new))
    steps = TWO * NT

    def rows_of(ref, g):
        return ref.at[g // NT, pl.ds(pl.multiple_of(lax.rem(g, NT) * TILE, TILE), TILE)]

    def tile_in(a, g):
        return pltpu.make_async_copy(rows_of(caches[a][0], g), caches[a][1].at[g], in_sem.at[a, g])

    def tile_out(a, g):
        return pltpu.make_async_copy(caches[a][1].at[g], rows_of(caches[a][2], g), out_sem.at[a, g])

    def tail_in(a, h):
        return pltpu.make_async_copy(caches[a][0].at[h, pl.ds(PAST, TOK)], caches[a][3].at[h], t_sem.at[0, a, h])

    def tail_out(a, h):
        return pltpu.make_async_copy(caches[a][3].at[h], caches[a][2].at[h, pl.ds(PAST, TOK)], t_sem.at[1, a, h])

    def win_at(h):
        s = start[h]
        return pl.multiple_of(jnp.minimum((s // 16) * 16, CACHE - WROWS), 16)

    def win_in(a, h):
        return pltpu.make_async_copy(caches[a][0].at[h, pl.ds(win_at(h), WROWS)], caches[a][4].at[h], w_sem.at[0, a, h])

    def win_out(a, h):
        return pltpu.make_async_copy(caches[a][4].at[h], caches[a][2].at[h, pl.ds(win_at(h), WROWS)], w_sem.at[1, a, h])

    local = ((kl, k0_new, kl_out), (vl, v0_new, vl_out))
    for a in PAIR:
        pltpu.make_async_copy(local[a][0], lbuf.at[a], l_sem.at[a]).start()
    for g in range(AHEAD):
        for a in PAIR:
            tile_in(a, g).start()
    for h in PAIR:
        for a in PAIR:
            win_in(a, h).start()
            tail_in(a, h).start()

    for a in PAIR:
        pltpu.make_async_copy(local[a][0], lbuf.at[a], l_sem.at[a]).wait()
        for h in PAIR:
            fresh = local[a][1][h].astype(F32)
            ext[0:TOK] = fresh
            ext[WIN:WIN + TOK] = fresh
            off = jnp.bitwise_and(-start[h], WIN - 1)

            def slots(b, _):
                rows = shifted(ext, off + b * 128, 128)
                age = jnp.bitwise_and(lax.broadcasted_iota(jnp.int32, (128, 1), 0) + (b * 128 + off), WIN - 1)
                at = pl.ds(pl.multiple_of(b * 128, 128), 128)
                lbuf[a, h, at, :] = jnp.where(age < TOK, rows, lbuf[a, h, at, :].astype(F32)).astype(BF)
                return 0

            lax.fori_loop(0, 8, slots, 0)
        pltpu.make_async_copy(lbuf.at[a], local[a][2], l_sem.at[a]).start()

    row = lax.broadcasted_iota(jnp.int32, (2 * TOK, 1), 0)
    qi = jnp.where(row >= TOK, row - TOK, row)

    def fetch(g):
        for a in PAIR:
            tile_in(a, g).wait()
            tile_out(a, g).start()

        @pl.when(g + AHEAD < steps)
        def _():
            for a in PAIR:
                tile_in(a, g + AHEAD).start()

    for h in PAIR:
        acc[...] = jnp.zeros_like(acc)
        tot[...] = jnp.zeros_like(tot)
        pb[...] = jnp.zeros_like(pb)
        base = h * NT

        def weigh(t, dst):
            for b in range(TILE // 256):
                scores = dot_t(q_in[h], kb[base + t, b * 256:(b + 1) * 256, :])
                slot = lax.broadcasted_iota(jnp.int32, (1, 256), 1) + (t * TILE + b * 256)
                off = jnp.where(slot < start[h], S_OFF, HIDE)
                wts = jnp.exp2(jnp.tanh(scores * S_IN) * S_OUT - off)
                tot[...] += wts[:, :128] + wts[:, 128:]
                dst[:, b * 256:(b + 1) * 256] = wts.astype(BF)

        def two_tiles(i, _):
            t = 2 * i
            fetch(base + t)
            fetch(base + t + 1)
            before = dot(pb[...], vb[base + jnp.maximum(t - 1, 0)])
            weigh(t, pa)
            now = dot(pa[...], vb[base + t])
            acc[...] += before + now
            weigh(t + 1, pb)
            return 0

        pairs = (start[h] + 2 * TILE - 1) // (2 * TILE)
        lax.fori_loop(0, pairs, two_tiles, 0)
        lax.fori_loop(2 * pairs, NT, lambda t, _: (fetch(base + t), 0)[1], 0)
        before = dot(pb[...], vb[base + 2 * pairs - 1])
        wts = jnp.where(lax.broadcasted_iota(jnp.int32, (1, TOK), 1) <= qi, soft_weights(dot_t(q_in[h], k_new[h])), 0.0)
        total = jnp.sum(tot[...], axis=-1, keepdims=True) + jnp.sum(wts, axis=-1, keepdims=True)
        o = ((acc[...] + before + dot(wts.astype(BF), v_new[h])) / total).astype(BF)
        obuf[h, :, :HD] = o[:TOK]
        obuf[h, :, HD:] = o[TOK:]

        for a in PAIR:
            tail_in(a, h).wait()
            tail_out(a, h).start()
            win_in(a, h).wait()
            ext[16:16 + TOK] = caches[a][5][h].astype(F32)
            shift = win_at(h) - start[h]
            rows = shifted(ext, shift + 16, WROWS)
            idx = lax.broadcasted_iota(jnp.int32, (WROWS, 1), 0) + shift
            win = caches[a][4]
            win[h] = jnp.where((idx >= 0) & (idx < TOK), rows, win[h].astype(F32)).astype(BF)

    done = pltpu.make_async_copy(obuf, o_out, l_sem.at[2])
    done.start()

    def drain(g, _):
        for a in PAIR:
            tile_out(a, g).wait()
        return 0

    lax.fori_loop(0, steps, drain, 0)
    for h in PAIR:
        for a in PAIR:
            tail_out(a, h).wait()
            win_out(a, h).start()
    done.wait()
    for a in PAIR:
        pltpu.make_async_copy(lbuf.at[a], local[a][2], l_sem.at[a]).wait()
        for h in PAIR:
            win_out(a, h).wait()


ANY = pl.BlockSpec(memory_space=pl.ANY)
VM = pl.BlockSpec(memory_space=pltpu.VMEM)
SM = pl.BlockSpec(memory_space=pltpu.SMEM)
DMA = pltpu.SemaphoreType.DMA


def vmem(*shape, dtype=BF):
    return pltpu.VMEM(shape, dtype)


def sds(*shape, dtype=BF):
    return jax.ShapeDtypeStruct(shape, dtype)


def run_first(start, invf, norms, x, kl, vl, *weights):
    return pl.pallas_call(
        first_kernel,
        name="first",
        out_shape=(sds(TWO, TWO * TOK, HD), sds(TWO, TOK, HD), sds(TWO, TOK, HD), sds(TWO, TWO, BLK, D), sds(TWO, TOK, HD), sds(TWO, TOK, HD)),
        in_specs=[SM, VM, VM] + [ANY] * 10,
        out_specs=(ANY,) * 6,
        scratch_shapes=[
            vmem(TWO, TWO, TWO, BLK, D), vmem(TWO, TWO, BLK, D), vmem(TWO, WIN, HD), vmem(TWO, WIN, HD), vmem(TWO * TOK, HD), vmem(TWO, TOK, HD), vmem(TWO, TOK, HD),
            vmem(TOK, 512), vmem(TWO, TOK, HALF), vmem(TWO, TWO, TWO, BLK, HALF, dtype=F32),
            vmem(TWO, TWO, TWO, BLK, HALF), vmem(TWO, TWO, TWO, BLK, HALF), vmem(TWO, TWO, TWO, BLK, HALF), vmem(TWO, TWO, TWO, TWO, BLK, HALF),
            vmem(TWO, D, HALF), vmem(TWO, D, HALF), vmem(TWO, D, HALF),
            vmem(TWO, TOK, 128, dtype=F32), vmem(TWO, TOK, 128, dtype=F32), vmem(TWO, TWO * TOK, HD),
            DMA((3, TWO, TWO)), DMA((TWO, TWO, TWO, TWO)), DMA((TWO, TWO, TWO, TWO)), DMA((TWO, TWO, TWO)), DMA((18,)), DMA((6,)),
        ],
        compiler_params=pltpu.CompilerParams(collective_id=0, has_side_effects=True, vmem_limit_bytes=VMEM_LIMIT),
    )(start, invf, norms, x, kl, vl, *weights)


def run_global(start, q, k_new, v_new, k0_new, v0_new, kl, vl, kg, vg):
    return pl.pallas_call(
        global_kernel,
        name="attend",
        out_shape=(sds(TWO, TOK, 512), sds(TWO, WIN, HD), sds(TWO, WIN, HD), sds(TWO, CACHE, HD), sds(TWO, CACHE, HD)),
        in_specs=[SM] + [VM] * 5 + [ANY] * 4,
        out_specs=(ANY,) * 5,
        scratch_shapes=[
            vmem(TWO * NT, TILE, HD), vmem(TWO * NT, TILE, HD), vmem(TWO, TOK, HD), vmem(TWO, TOK, HD), vmem(TWO, WROWS, HD), vmem(TWO, WROWS, HD),
            vmem(TWO, TWO, WIN, HD), vmem(TWO * WIN + 8, HD, dtype=F32), vmem(TWO * TOK, TILE), vmem(TWO * TOK, TILE), vmem(TWO * TOK, HD, dtype=F32),
            vmem(TWO * TOK, 128, dtype=F32), vmem(TWO, TOK, 512),
            DMA((TWO, TWO * NT)), DMA((TWO, TWO * NT)), DMA((TWO, TWO, TWO)), DMA((TWO, TWO, TWO)), DMA((3,)),
        ],
        compiler_params=pltpu.CompilerParams(has_side_effects=True, vmem_limit_bytes=VMEM_LIMIT),
    )(start, q, k_new, v_new, k0_new, v0_new, kl, vl, kg, vg)


def run_last(norms, o, x, wo, wg, wu, wd):
    return pl.pallas_call(
        last_kernel,
        name="last",
        out_shape=sds(TWO, BLK, D),
        in_specs=[VM] + [ANY] * 6,
        out_specs=VM,
        scratch_shapes=[
            vmem(TWO, TWO, TWO, BLK, D), vmem(TWO, TWO, BLK, D), vmem(TWO, TOK, 512), vmem(TWO, TOK, HALF), vmem(TWO, TWO, TWO, BLK, HALF, dtype=F32),
            vmem(TWO, TWO, TWO, BLK, HALF), vmem(TWO, TWO, TWO, BLK, HALF), vmem(TWO, TWO, TWO, BLK, HALF), vmem(TWO, TWO, TWO, BLK, HALF), vmem(TWO, TWO, BLK, HALF),
            vmem(TWO, 512, HALF), vmem(TWO, D, HALF), vmem(TWO, D, HALF), vmem(TWO, D, HALF),
            DMA((TWO, TWO, TWO, TWO)), DMA((TWO, TWO, TWO, TWO)), DMA((TWO, TWO)), DMA((10,)),
        ],
        compiler_params=pltpu.CompilerParams(collective_id=1, has_side_effects=True, vmem_limit_bytes=VMEM_LIMIT),
    )(norms, o, x, wo, wg, wu, wd)


def solution(mesh):
    act_spec = P('dp', 'tp', None)
    cache_spec = P('dp', None, 'tp', None)
    col_spec = P(None, None, 'tp')
    row_spec = P(None, 'tp', None)
    arg_specs = (act_spec, P('dp'), cache_spec, cache_spec, cache_spec, cache_spec, P(), col_spec, col_spec, col_spec, row_spec, col_spec, col_spec, row_spec)
    result_specs = (act_spec, cache_spec, cache_spec, cache_spec, cache_spec)
    inv_freq = np.power(np.float64(ROPE_BASE), np.arange(HD // 2) * (-2.0 / HD)).astype(np.float32)[None, :]

    def device_step(x, start, k_local, v_local, k_global, v_global, norms, w_q, w_k, w_v, w_o, w_gate, w_up, w_down):
        def flat(cache):
            return cache.reshape(cache.shape[0], cache.shape[1], cache.shape[3])

        kl, vl, kg, vg = flat(k_local), flat(v_local), flat(k_global), flat(v_global)
        q1, k1, v1, xres, k0, v0 = run_first(start, jnp.asarray(inv_freq), norms, x, kl, vl, w_q, w_k, w_v, w_o, w_gate, w_up, w_down)
        o1, kl_new, vl_new, kg_new, vg_new = run_global(start, q1, k1, v1, k0, v0, kl, vl, kg, vg)
        out = run_last(norms, o1, xres, w_o, w_gate, w_up, w_down)
        return (out, kl_new.reshape(k_local.shape), vl_new.reshape(v_local.shape), kg_new.reshape(k_global.shape), vg_new.reshape(v_global.shape))

    return jax.shard_map(device_step, mesh=mesh, in_specs=arg_specs, out_specs=result_specs, check_vma=False)
```

```python
import functools

import jax
import jax.numpy as jnp
import numpy as np
from jax import lax
from jax.experimental import pallas as pl
from jax.experimental.pallas import tpu as pltpu
from jax.sharding import PartitionSpec as P

BF = jnp.bfloat16
F32 = jnp.float32
MESH = pl.DeviceIdType.MESH
NORM_EPS = 1e-6
ROPE_BASE = 10000.0
LOG2E = 1.4426950408889634
S_IN = 1.0 / (50.0 * 16.0)
S_OUT = 50.0 * LOG2E
S_OFF = 36.0 * LOG2E

D = 2560
HALF = 1280
TOK = 192
BLK = 48
HD = 256
WIN = 1024
VMEM_LIMIT = 67000000
TWO = 2
PAIR = range(TWO)
GROUPS = tuple(slice(i, i + 16) for i in range(0, BLK, 16))


TILE = 1024
PAST = 12288
CACHE = PAST + TOK
NT = PAST // TILE
WROWS = TOK + 16
AHEAD = 5
HIDE = 1e6


def dot(a, b):
    return jnp.dot(a, b, preferred_element_type=F32)


def dot_t(a, b):
    return lax.dot_general(a, b, (((1,), (1,)), ((), ())), preferred_element_type=F32)


def soft_weights(scores):
    return jnp.exp2(jnp.tanh(scores * S_IN) * S_OUT - S_OFF)


def rope_into(proj, cos, sin, q_dst, k_dst):
    for head, (ref, row) in enumerate(((q_dst, 0), (q_dst, TOK), (k_dst, 0))):
        lead = proj[:, head * HD:head * HD + 128]
        tail = proj[:, head * HD + 128:(head + 1) * HD]
        ref[row:row + TOK, :128] = (lead * cos - tail * sin).astype(BF)
        ref[row:row + TOK, 128:] = (tail * cos + lead * sin).astype(BF)


class Peers:
    def __init__(self):
        dp = lax.axis_index("dp")
        tp = lax.axis_index("tp")
        self.x = tp // 2
        self.c = lax.rem(tp, 2)
        self.mate = (dp, tp + 1 - 2 * self.c)
        self.far = (dp, lax.rem(tp + 2, 4))

    def barrier(self):
        sem = pltpu.get_barrier_semaphore()
        for peer in (self.mate, self.far):
            pl.semaphore_signal(sem, inc=1, device_id=peer, device_id_type=MESH)
        pl.semaphore_wait(sem, 2)


def remote(src, dst, send, recv, peer):
    return pltpu.make_async_remote_copy(src_ref=src, dst_ref=dst, send_sem=send, recv_sem=recv, device_id=peer, device_id_type=MESH)


def norm_rows(act, h, w):
    def body(i, _):
        for r in GROUPS:
            rows = act[h, i // 2, i % 2, r, :].astype(F32)
            inv = lax.rsqrt(jnp.sum(rows * rows, axis=-1, keepdims=True) * (1.0 / D) + NORM_EPS)
            act[h, i // 2, i % 2, r, :] = (rows * inv * w).astype(BF)
        return 0
    lax.fori_loop(0, 4, body, 0)


class Exchange:
    def __init__(self, peers, pbuf, ds, dr, es, er, d_sem, e_sem):
        self.p, self.pbuf, self.ds, self.dr, self.es, self.er = peers, pbuf, ds, dr, es, er
        self.d_sem, self.e_sem = d_sem, e_sem

    def d_copy(self, h, n):
        return remote(self.ds.at[h, n], self.dr.at[h, n], self.d_sem.at[0, h, n], self.d_sem.at[1, h, n], self.p.mate)

    def e_copy(self, h, n):
        return remote(self.es.at[h, n], self.er.at[h, n], self.e_sem.at[0, h, n], self.e_sem.at[1, h, n], self.p.far)

    def give(self, h, n, part):
        self.pbuf[n] = part.reshape(2, 2, BLK, HALF)
        self.ds[h, n] = self.pbuf[n, :, 1 - self.p.c].astype(BF)
        self.d_copy(h, n).start()

    def send(self, h, n):
        copy = self.d_copy(h, n)
        copy.wait_recv()
        self.es[h, n] = (self.pbuf[n, :, self.p.c] + self.dr[h, n].astype(F32)).astype(BF)
        self.e_copy(h, n).start()
        copy.wait_send()

    def take(self, h, xres, w_post, act, w_pre):
        for n in PAIR:
            self.e_copy(h, n).wait()
        c = self.p.c

        def body(xb, _):
            for r in GROUPS:
                ys = [(self.es[h, n, xb, r, :].astype(F32) + self.er[h, n, xb, r, :].astype(F32)).astype(BF).astype(F32) for n in PAIR]
                inv = lax.rsqrt(sum(jnp.sum(y * y, axis=-1, keepdims=True) for y in ys) * (1.0 / D) + NORM_EPS)
                news = []
                for n in PAIR:
                    cols = slice(n * HALF, (n + 1) * HALF)
                    new = (xres[h, xb, r, cols].astype(F32) + ys[n] * inv * w_post[:, cols]).astype(BF)
                    xres[h, xb, r, cols] = new
                    news.append(new.astype(F32))
                inv = lax.rsqrt(sum(jnp.sum(v * v, axis=-1, keepdims=True) for v in news) * (1.0 / D) + NORM_EPS)
                for n in PAIR:
                    cols = slice(n * HALF, (n + 1) * HALF)
                    act[h, xb, c, r, cols] = (news[n] * inv * w_pre[:, cols]).astype(BF)
            return 0
        lax.fori_loop(0, 2, body, 0)


class Final:
    def __init__(self, peers, pbuf, ds, dr, es, er, d_sem, e_sem):
        self.p, self.pbuf, self.ds, self.dr, self.es, self.er = peers, pbuf, ds, dr, es, er
        self.d_sem, self.e_sem = d_sem, e_sem

    d_copy = Exchange.d_copy
    give = Exchange.give

    def e_copy(self, h, n):
        return remote(self.es.at[h, n, 1 - self.p.x], self.er.at[h, n, 0], self.e_sem.at[0, h, n], self.e_sem.at[1, h, n], self.p.far)

    send = Exchange.send

    def take(self, h, xres, w_post, out):
        for n in PAIR:
            self.e_copy(h, n).wait()
        x = self.p.x

        for r in GROUPS:
            ys = [(self.es[h, n, x, r, :].astype(F32) + self.er[h, n, 0, r, :].astype(F32)).astype(BF).astype(F32) for n in PAIR]
            inv = lax.rsqrt(sum(jnp.sum(y * y, axis=-1, keepdims=True) for y in ys) * (1.0 / D) + NORM_EPS)
            for n in PAIR:
                cols = slice(n * HALF, (n + 1) * HALF)
                out[h, r, cols] = (xres[h, x, r, cols].astype(F32) + ys[n] * inv * w_post[:, cols]).astype(BF)


class Shared:
    def __init__(self, peers, act, sem):
        self.p, self.act, self.sem = peers, act, sem

    def copy(self, h):
        view = self.act.at[h, :, self.p.c]
        return remote(view, view, self.sem.at[0, h], self.sem.at[1, h], self.p.mate)


def load(src, dst, sem):
    copy = pltpu.make_async_copy(src, dst, sem)
    copy.start()
    return copy


def load_mlp(layer, w, buf, sems):
    return [load(w.at[layer, :, pl.ds(n * HALF, HALF)], buf.at[n], sems.at[n]) for n in PAIR]


def gate_up(act, h, wg, wu, hid):
    def body(n, _):
        g = act[h].reshape(TOK, D)
        gate = dot(g, wg[n])
        up = dot(g, wu[n])
        hid[n] = (jax.nn.gelu(gate, approximate=True) * up).astype(BF)
        return 0
    lax.fori_loop(0, 2, body, 0)


def down(hid, wd, n):
    return dot(hid[0], wd[n, :HALF]) + dot(hid[1], wd[n, HALF:])


def layers_kernel(start, invf, norms, x_in, kl, vl, kg, vg, wq, wk, wv, wo, wg, wu, wd,
                  out_ref, k0_out, v0_out, k1_out, v1_out,
                  act, xres, kc, vc, qs, ks, vs, obuf, hid, pbuf, ds, dr, es, er, wgb, wub, wdb, wob, cosb, sinb, pa, pb, acc, tot,
                  ag_sem, d_sem, e_sem, g_sem, w_sem, o_sem, t_sem):
    p = Peers()
    loads = [load(wq.at[0], wdb.at[0, :, pl.ds(0, 512)], w_sem.at[0]),
             load(wk.at[0], wdb.at[0, :, pl.ds(512, 256)], w_sem.at[1]),
             load(wv.at[0], wdb.at[0, :, pl.ds(768, 256)], w_sem.at[2]),
             load(kl, kc, w_sem.at[3]),
             load(vl, vc, w_sem.at[4])]
    load_o = [load(wo.at[0, :, pl.ds(n * HALF, HALF)], wdb.at[1, pl.ds(n * 512, 512), :], w_sem.at[5 + n]) for n in PAIR]
    own = [load(x_in.at[h], act.at[h, p.x, p.c], w_sem.at[7 + h]) for h in PAIR]
    p.barrier()

    def ag_mate(h):
        return remote(x_in.at[h], act.at[h, p.x, p.c], ag_sem.at[0, 0, h], ag_sem.at[0, 1, h], p.mate)

    def ag_far(h):
        return remote(x_in.at[h], act.at[h, p.x, p.c], ag_sem.at[1, 0, h], ag_sem.at[1, 1, h], p.far)

    def ag_pass(h):
        view = act.at[h, 1 - p.x, p.c]
        return remote(view, view, ag_sem.at[2, 0, h], ag_sem.at[2, 1, h], p.mate)

    for h in PAIR:
        ag_far(h).start()
        ag_mate(h).start()
    for h in PAIR:
        pos = (lax.broadcasted_iota(jnp.int32, (TOK, 128), 0) + start[h]).astype(F32)
        angle = pos * invf[...]
        cosb[h] = jnp.cos(angle)
        sinb[h] = jnp.sin(angle)

    w0 = 1.0 + norms[0]
    w1 = 1.0 + norms[1]

    def ag_arrive(h):
        ag_far(h).wait_recv()
        ag_pass(h).start()

    def ag_finish(h):
        own[h].wait()
        ag_mate(h).wait_recv()
        ag_pass(h).wait()
        ag_mate(h).wait_send()
        ag_far(h).wait_send()
        xres[h] = act[h, :, p.c]
        norm_rows(act, h, w0[0:1])

    def local_attention(h):
        q = qs[...]
        row = lax.broadcasted_iota(jnp.int32, (2 * TOK, 1), 0)
        i = jnp.where(row >= TOK, row - TOK, row)
        least = jnp.maximum(i + 1, WIN - start[h])
        acc = jnp.zeros((2 * TOK, HD), F32)
        total = jnp.zeros((2 * TOK, 1), F32)
        for b in PAIR:
            slot = lax.broadcasted_iota(jnp.int32, (1, 512), 1) + b * 512
            age = jnp.bitwise_and(slot - start[h], WIN - 1)
            wts = jnp.where(age >= least, soft_weights(dot_t(q, kc[h, b * 512:(b + 1) * 512, :])), 0.0)
            total += jnp.sum(wts, axis=-1, keepdims=True)
            acc += dot(wts.astype(BF), vc[h, b * 512:(b + 1) * 512, :])
        key = lax.broadcasted_iota(jnp.int32, (1, TOK), 1)
        wts = jnp.where(key <= i, soft_weights(dot_t(q, ks[h])), 0.0)
        total += jnp.sum(wts, axis=-1, keepdims=True)
        acc += dot(wts.astype(BF), vs[h])
        o = (acc / total).astype(BF)
        obuf[:, :HD] = o[:TOK]
        obuf[:, HD:] = o[TOK:]

    ex = [Exchange(p, pbuf, ds, dr, es, er.at[s % 2], d_sem.at[s], e_sem.at[s]) for s in range(3)]
    ex.append(Final(p, pbuf, ds, dr, es, er.at[1], d_sem.at[3], e_sem.at[3]))
    sh = [Shared(p, act, g_sem.at[s]) for s in range(3)]

    for h in PAIR:
        if h == 0:
            ag_arrive(0)
        ag_finish(h)
        if h == 0:
            for copy in loads + load_o:
                copy.wait()
            load_g = load_mlp(0, wg, wgb, w_sem.at[pl.ds(9, 2)])
            load_u = load_mlp(0, wu, wub, w_sem.at[pl.ds(11, 2)])
        proj = dot(act[h].reshape(TOK, D), wdb[0, :, :1024])
        rope_into(proj, cosb[h], sinb[h], qs, ks.at[h])
        vs[h] = proj[:, 768:].astype(BF)
        local_attention(h)
        for n in PAIR:
            ex[0].give(h, n, dot(obuf[...], wdb[1, n * 512:(n + 1) * 512, :]))
        if h == 0:
            ag_arrive(1)
        for n in PAIR:
            ex[0].send(h, n)
    load_d = load_mlp(0, wd, wdb, w_sem.at[pl.ds(13, 2)])
    outs = [load(ks, k0_out, o_sem.at[0]), load(vs, v0_out, o_sem.at[1])]

    def mlp(before, after, share, w_post, w_pre, first_loads, last_loads):
        def body(h, _):
            before.take(h, xres, w_post, act, w_pre)
            share.copy(h).start()

            @pl.when(h == 1)
            def _():
                after.send(0, 1)

            share.copy(h).wait()

            @pl.when(h == 0)
            def _():
                for copy in first_loads:
                    copy.wait()

            gate_up(act, h, wgb, wub, hid)

            @pl.when(h == 0)
            def _():
                for copy in last_loads:
                    copy.wait()

            for n in PAIR:
                after.give(h, n, down(hid, wdb, n))
            after.send(h, 0)
            return 0

        lax.fori_loop(0, 2, body, 0)

    mlp(ex[0], ex[1], sh[0], w0[1:2], w0[2:3], load_g + load_u, load_d)

    loads = [load(wq.at[1], wgb.at[0, :, pl.ds(0, 512)], w_sem.at[15]),
             load(wk.at[1], wgb.at[0, :, pl.ds(512, 256)], w_sem.at[16]),
             load(wv.at[1], wgb.at[0, :, pl.ds(768, 256)], w_sem.at[17])]

    def ring(a, g):
        s = lax.rem(g, 8)
        return wdb.at[s // 4, pl.ds(a * TILE, TILE), pl.ds(pl.multiple_of(lax.rem(s, 4) * HD, HD), HD)]

    def tile_in(a, g):
        src = (kg, vg)[a].at[g // NT, pl.ds(pl.multiple_of(lax.rem(g, NT) * TILE, TILE), TILE)]
        return pltpu.make_async_copy(src, ring(a, g), t_sem.at[a, g])

    for g in range(AHEAD):
        for a in PAIR:
            tile_in(a, g).start()
    load_o1 = [load(wo.at[1, :, pl.ds(n * HALF, HALF)], wob.at[n], w_sem.at[18 + n]) for n in PAIR]
    load_u1 = load_mlp(1, wu, wub, w_sem.at[pl.ds(11, 2)])
    load_g1 = [pltpu.make_async_copy(wg.at[1, :, pl.ds(n * HALF, HALF)], wgb.at[n], w_sem.at[9 + n]) for n in PAIR]

    def fetch(g):
        for a in PAIR:
            tile_in(a, g).wait()

        @pl.when(g + AHEAD < TWO * NT)
        def _():
            for a in PAIR:
                tile_in(a, g + AHEAD).start()

    row = lax.broadcasted_iota(jnp.int32, (2 * TOK, 1), 0)
    qi = jnp.where(row >= TOK, row - TOK, row)

    def global_attention(h):
        acc[...] = jnp.zeros_like(acc)
        tot[...] = jnp.zeros_like(tot)
        pb[...] = jnp.zeros_like(pb)
        base = h * NT

        def weigh(t, dst):
            keys = ring(0, base + t)
            for b in range(TILE // 256):
                scores = dot_t(qs[...], keys[b * 256:(b + 1) * 256, :])
                slot = lax.broadcasted_iota(jnp.int32, (1, 256), 1) + (t * TILE + b * 256)
                off = jnp.where(slot < start[h], S_OFF, HIDE)
                wts = jnp.exp2(jnp.tanh(scores * S_IN) * S_OUT - off)
                tot[...] += wts[:, :128] + wts[:, 128:]
                dst[:, b * 256:(b + 1) * 256] = wts.astype(BF)

        def two_tiles(i, _):
            t = 2 * i
            fetch(base + t)
            fetch(base + t + 1)
            before = dot(pb[...], ring(1, base + jnp.maximum(t - 1, 0))[...])
            weigh(t, pa)
            now = dot(pa[...], ring(1, base + t)[...])
            acc[...] += before + now
            weigh(t + 1, pb)
            return 0

        lax.fori_loop(0, NT // 2, two_tiles, 0)
        before = dot(pb[...], ring(1, base + NT - 1)[...])
        wts = jnp.where(lax.broadcasted_iota(jnp.int32, (1, TOK), 1) <= qi, soft_weights(dot_t(qs[...], ks[h])), 0.0)
        total = jnp.sum(tot[...], axis=-1, keepdims=True) + jnp.sum(wts, axis=-1, keepdims=True)
        o = ((acc[...] + before + dot(wts.astype(BF), vs[h])) / total).astype(BF)
        obuf[:, :HD] = o[:TOK]
        obuf[:, HD:] = o[TOK:]

    def attend(h, _):
        ex[1].take(h, xres, w0[3:4], act, w1[0:1])
        sh[1].copy(h).start()

        @pl.when(h == 0)
        def _():
            ex[1].send(1, 1)
            for copy in outs + loads + load_o1:
                copy.wait()

        sh[1].copy(h).wait()
        proj = dot(act[h].reshape(TOK, D), wgb[0, :, :1024])
        rope_into(proj, cosb[h], sinb[h], qs, ks.at[h])
        vs[h] = proj[:, 768:].astype(BF)

        @pl.when(h == 1)
        def _():
            for copy in load_g1:
                copy.start()

        global_attention(h)
        for n in PAIR:
            ex[2].give(h, n, dot(obuf[...], wob[n]))
        for n in PAIR:
            ex[2].send(h, n)
        return 0

    lax.fori_loop(0, 2, attend, 0)
    outs = [load(ks, k1_out, o_sem.at[2]), load(vs, v1_out, o_sem.at[3])]
    load_d1 = load_mlp(1, wd, wdb, w_sem.at[pl.ds(13, 2)])
    mlp(ex[2], ex[3], sh[2], w1[1:2], w1[2:3], load_u1 + load_g1, load_d1)
    ex[3].send(1, 1)
    for h in PAIR:
        ex[3].take(h, xres, w1[3:4], out_ref)
    for copy in outs:
        copy.wait()


def shifted(ref, off, n):
    base = pl.multiple_of((off // 8) * 8, 8)
    rows = ref[pl.ds(base, n + 8), :]
    return pltpu.roll(rows, lax.rem(n + 8 - (off - base), n + 8), 0)[:n]


def cache_kernel(start, k_new, v_new, k0_new, v0_new, kl, vl, kg, vg,
                 kl_out, vl_out, kg_out, vg_out,
                 kb, vb, kt, vt, kwin, vwin, lbuf, ext, in_sem, out_sem, t_sem, w_sem, l_sem):
    caches = ((kg, kb, kg_out, kt, kwin, k_new), (vg, vb, vg_out, vt, vwin, v_new))
    steps = TWO * NT

    def rows_of(ref, g):
        return ref.at[g // NT, pl.ds(pl.multiple_of(lax.rem(g, NT) * TILE, TILE), TILE)]

    def tile_in(a, g):
        return pltpu.make_async_copy(rows_of(caches[a][0], g), caches[a][1].at[g], in_sem.at[a, g])

    def tile_out(a, g):
        return pltpu.make_async_copy(caches[a][1].at[g], rows_of(caches[a][2], g), out_sem.at[a, g])

    def tail_in(a, h):
        return pltpu.make_async_copy(caches[a][0].at[h, pl.ds(PAST, TOK)], caches[a][3].at[h], t_sem.at[0, a, h])

    def tail_out(a, h):
        return pltpu.make_async_copy(caches[a][3].at[h], caches[a][2].at[h, pl.ds(PAST, TOK)], t_sem.at[1, a, h])

    def win_at(h):
        s = start[h]
        return pl.multiple_of(jnp.minimum((s // 16) * 16, CACHE - WROWS), 16)

    def win_in(a, h):
        return pltpu.make_async_copy(caches[a][0].at[h, pl.ds(win_at(h), WROWS)], caches[a][4].at[h], w_sem.at[0, a, h])

    def win_out(a, h):
        return pltpu.make_async_copy(caches[a][4].at[h], caches[a][2].at[h, pl.ds(win_at(h), WROWS)], w_sem.at[1, a, h])

    local = ((kl, k0_new, kl_out), (vl, v0_new, vl_out))
    for a in PAIR:
        pltpu.make_async_copy(local[a][0], lbuf.at[a], l_sem.at[a]).start()
    for h in PAIR:
        for a in PAIR:
            win_in(a, h).start()
            tail_in(a, h).start()

    def begin(g, _):
        for a in PAIR:
            tile_in(a, g).start()
        return 0

    lax.fori_loop(0, steps, begin, 0)

    def move(g, _):
        for a in PAIR:
            tile_in(a, g).wait()
            tile_out(a, g).start()
        return 0

    def local_rows(a, h):
        fresh = local[a][1][h].astype(F32)
        ext[0:TOK] = fresh
        ext[WIN:WIN + TOK] = fresh
        off = jnp.bitwise_and(-start[h], WIN - 1)

        def slots(b, _):
            lead = jnp.bitwise_and(b * 128 + off, WIN - 1)

            @pl.when((lead < TOK) | (lead > WIN - 128))
            def _():
                rows = shifted(ext, off + b * 128, 128)
                age = jnp.bitwise_and(lax.broadcasted_iota(jnp.int32, (128, 1), 0) + lead, WIN - 1)
                at = pl.ds(pl.multiple_of(b * 128, 128), 128)
                lbuf[a, h, at, :] = jnp.where(age < TOK, rows, lbuf[a, h, at, :].astype(F32)).astype(BF)

            return 0

        lax.fori_loop(0, WIN // 128, slots, 0)

    def global_rows(a, h):
        win_in(a, h).wait()
        ext[16:16 + TOK] = caches[a][5][h].astype(F32)
        shift = win_at(h) - start[h]
        rows = shifted(ext, shift + 16, WROWS)
        idx = lax.broadcasted_iota(jnp.int32, (WROWS, 1), 0) + shift
        win = caches[a][4]
        win[h] = jnp.where((idx >= 0) & (idx < TOK), rows, win[h].astype(F32)).astype(BF)

    for a in PAIR:
        pltpu.make_async_copy(local[a][0], lbuf.at[a], l_sem.at[a]).wait()
        for h in PAIR:
            i = TWO * a + h
            local_rows(a, h)
            lax.fori_loop(i * 3, i * 3 + 3, move, 0)
        pltpu.make_async_copy(lbuf.at[a], local[a][2], l_sem.at[a]).start()
    for a in PAIR:
        for h in PAIR:
            i = TWO * a + h
            tail_in(a, h).wait()
            tail_out(a, h).start()
            global_rows(a, h)
            lax.fori_loop(NT + i * 3, NT + i * 3 + 3, move, 0)

    def drain(g, _):
        for a in PAIR:
            tile_out(a, g).wait()
        return 0

    for h in PAIR:
        lax.fori_loop(h * NT, h * NT + NT, drain, 0)
        for a in PAIR:
            tail_out(a, h).wait()
            win_out(a, h).start()
    for a in PAIR:
        pltpu.make_async_copy(lbuf.at[a], local[a][2], l_sem.at[a]).wait()
        for h in PAIR:
            win_out(a, h).wait()


ANY = pl.BlockSpec(memory_space=pl.ANY)
VM = pl.BlockSpec(memory_space=pltpu.VMEM)
SM = pl.BlockSpec(memory_space=pltpu.SMEM)
DMA = pltpu.SemaphoreType.DMA


def vmem(*shape, dtype=BF):
    return pltpu.VMEM(shape, dtype)


def sds(*shape, dtype=BF):
    return jax.ShapeDtypeStruct(shape, dtype)


def run_layers(start, invf, norms, x, kl, vl, kg, vg, *weights):
    rows = sds(TWO, TOK, HD)
    pieces = vmem(TWO, TWO, TWO, BLK, HALF)
    return pl.pallas_call(
        layers_kernel,
        name="layers",
        out_shape=(sds(TWO, BLK, D), rows, rows, rows, rows),
        in_specs=[SM, VM, VM] + [ANY] * 12,
        out_specs=(VM, ANY, ANY, ANY, ANY),
        scratch_shapes=[
            vmem(TWO, TWO, TWO, BLK, D), vmem(TWO, TWO, BLK, D), vmem(TWO, WIN, HD), vmem(TWO, WIN, HD),
            vmem(TWO * TOK, HD), vmem(TWO, TOK, HD), vmem(TWO, TOK, HD),
            vmem(TOK, 512), vmem(TWO, TOK, HALF), vmem(TWO, TWO, TWO, BLK, HALF, dtype=F32),
            pieces, pieces, pieces, vmem(TWO, TWO, TWO, TWO, BLK, HALF),
            vmem(TWO, D, HALF), vmem(TWO, D, HALF), vmem(TWO, D, HALF), vmem(TWO, 512, HALF),
            vmem(TWO, TOK, 128, dtype=F32), vmem(TWO, TOK, 128, dtype=F32),
            vmem(TWO * TOK, TILE), vmem(TWO * TOK, TILE), vmem(TWO * TOK, HD, dtype=F32), vmem(TWO * TOK, 128, dtype=F32),
            DMA((3, TWO, TWO)), DMA((4, TWO, TWO, TWO)), DMA((4, TWO, TWO, TWO)), DMA((3, TWO, TWO)), DMA((20,)), DMA((4,)),
            DMA((TWO, TWO * NT)),
        ],
        compiler_params=pltpu.CompilerParams(collective_id=0, has_side_effects=True, vmem_limit_bytes=VMEM_LIMIT),
    )(start, invf, norms, x, kl, vl, kg, vg, *weights)


def run_caches(start, k_new, v_new, k0_new, v0_new, kl, vl, kg, vg):
    tiles = vmem(TWO * NT, TILE, HD)
    window = vmem(TWO, WROWS, HD)
    return pl.pallas_call(
        cache_kernel,
        name="caches",
        out_shape=(sds(TWO, WIN, HD), sds(TWO, WIN, HD), sds(TWO, CACHE, HD), sds(TWO, CACHE, HD)),
        in_specs=[SM] + [VM] * 4 + [ANY] * 4,
        out_specs=(ANY,) * 4,
        scratch_shapes=[
            tiles, tiles, vmem(TWO, TOK, HD), vmem(TWO, TOK, HD), window, window,
            vmem(TWO, TWO, WIN, HD), vmem(TWO * WIN + 8, HD, dtype=F32),
            DMA((TWO, TWO * NT)), DMA((TWO, TWO * NT)), DMA((TWO, TWO, TWO)), DMA((TWO, TWO, TWO)), DMA((TWO,)),
        ],
        compiler_params=pltpu.CompilerParams(has_side_effects=True, vmem_limit_bytes=VMEM_LIMIT),
    )(start, k_new, v_new, k0_new, v0_new, kl, vl, kg, vg)


def solution(mesh):
    act_spec = P('dp', 'tp', None)
    cache_spec = P('dp', None, 'tp', None)
    col_spec = P(None, None, 'tp')
    row_spec = P(None, 'tp', None)
    arg_specs = (act_spec, P('dp'), cache_spec, cache_spec, cache_spec, cache_spec, P(), col_spec, col_spec, col_spec, row_spec, col_spec, col_spec, row_spec)
    result_specs = (act_spec, cache_spec, cache_spec, cache_spec, cache_spec)
    inv_freq = np.power(np.float64(ROPE_BASE), np.arange(HD // 2) * (-2.0 / HD)).astype(np.float32)[None, :]

    def device_step(x, start, k_local, v_local, k_global, v_global, norms, w_q, w_k, w_v, w_o, w_gate, w_up, w_down):
        def flat(cache):
            return cache.reshape(cache.shape[0], cache.shape[1], cache.shape[3])

        kl, vl, kg, vg = flat(k_local), flat(v_local), flat(k_global), flat(v_global)
        invf = jnp.asarray(inv_freq)
        out, k0, v0, k1, v1 = run_layers(start, invf, norms, x, kl, vl, kg, vg, w_q, w_k, w_v, w_o, w_gate, w_up, w_down)
        kl_new, vl_new, kg_new, vg_new = run_caches(start, k1, v1, k0, v0, kl, vl, kg, vg)
        return (out, kl_new.reshape(k_local.shape), vl_new.reshape(v_local.shape), kg_new.reshape(k_global.shape), vg_new.reshape(v_global.shape))

    return jax.shard_map(device_step, mesh=mesh, in_specs=arg_specs, out_specs=result_specs, check_vma=False)
```

```python
import functools

import jax
import jax.numpy as jnp
import numpy as np
from jax import lax
from jax.experimental import pallas as pl
from jax.experimental.pallas import tpu as pltpu
from jax.sharding import PartitionSpec as P

BF = jnp.bfloat16
F32 = jnp.float32
MESH = pl.DeviceIdType.MESH
NORM_EPS = 1e-6
ROPE_BASE = 10000.0
LOG2E = 1.4426950408889634
S_IN = 1.0 / (50.0 * 16.0)
S_OUT = 50.0 * LOG2E
S_OFF = 36.0 * LOG2E

D = 2560
HALF = 1280
TOK = 192
BLK = 48
HD = 256
WIN = 1024
VMEM_LIMIT = 67000000
TWO = 2
PAIR = range(TWO)
GROUPS = tuple(slice(i, i + 16) for i in range(0, BLK, 16))


TILE = 1024
PAST = 12288
CACHE = PAST + TOK
NT = PAST // TILE
WROWS = TOK + 16
AHEAD = 5
HIDE = 1e6


def dot(a, b):
    return jnp.dot(a, b, preferred_element_type=F32)


def dot_t(a, b):
    return lax.dot_general(a, b, (((1,), (1,)), ((), ())), preferred_element_type=F32)


def soft_weights(scores):
    return jnp.exp2(jnp.tanh(scores * S_IN) * S_OUT - S_OFF)


def rope_into(proj, cos, sin, q_dst, k_dst):
    for head, (ref, row) in enumerate(((q_dst, 0), (q_dst, TOK), (k_dst, 0))):
        lead = proj[:, head * HD:head * HD + 128]
        tail = proj[:, head * HD + 128:(head + 1) * HD]
        ref[row:row + TOK, :128] = (lead * cos - tail * sin).astype(BF)
        ref[row:row + TOK, 128:] = (tail * cos + lead * sin).astype(BF)


class Peers:
    def __init__(self):
        dp = lax.axis_index("dp")
        tp = lax.axis_index("tp")
        self.x = tp // 2
        self.c = lax.rem(tp, 2)
        self.mate = (dp, tp + 1 - 2 * self.c)
        self.far = (dp, lax.rem(tp + 2, 4))

    def barrier(self):
        sem = pltpu.get_barrier_semaphore()
        for peer in (self.mate, self.far):
            pl.semaphore_signal(sem, inc=1, device_id=peer, device_id_type=MESH)
        pl.semaphore_wait(sem, 2)


def remote(src, dst, send, recv, peer):
    return pltpu.make_async_remote_copy(src_ref=src, dst_ref=dst, send_sem=send, recv_sem=recv, device_id=peer, device_id_type=MESH)


def norm_rows(act, h, w):
    def body(i, _):
        for r in GROUPS:
            rows = act[h, i // 2, i % 2, r, :].astype(F32)
            inv = lax.rsqrt(jnp.sum(rows * rows, axis=-1, keepdims=True) * (1.0 / D) + NORM_EPS)
            act[h, i // 2, i % 2, r, :] = (rows * inv * w).astype(BF)
        return 0
    lax.fori_loop(0, 4, body, 0)


class Exchange:
    def __init__(self, peers, pbuf, ds, dr, es, er, d_sem, e_sem, final=None):
        self.p, self.pbuf, self.ds, self.dr, self.es, self.er = peers, pbuf, ds, dr, es, er
        self.d_sem, self.e_sem, self.final = d_sem, e_sem, final

    def d_copy(self, h, n):
        return remote(self.ds.at[h, n], self.dr.at[h, n], self.d_sem.at[0, h, n], self.d_sem.at[1, h, n], self.p.mate)

    def e_copy(self, h, n):
        return remote(self.es.at[h, n], self.er.at[h, n], self.e_sem.at[0, h, n], self.e_sem.at[1, h, n], self.p.far)

    def give(self, h, n, part):
        self.pbuf[n] = part.reshape(2, 2, BLK, HALF)
        self.ds[h, n] = self.pbuf[n, :, 1 - self.p.c].astype(BF)
        self.d_copy(h, n).start()

    def send(self, h, n):
        copy = self.d_copy(h, n)
        copy.wait_recv()
        self.es[h, n] = (self.pbuf[n, :, self.p.c] + self.dr[h, n].astype(F32)).astype(BF)
        if self.final is None:
            self.e_copy(h, n).start()
        else:
            pl.when(self.final)(lambda: self.f_copy(h, n).start())
            pl.when(jnp.logical_not(self.final))(lambda: self.e_copy(h, n).start())
        copy.wait_send()

    def f_copy(self, h, n):
        return remote(self.es.at[h, n, 1 - self.p.x], self.er.at[h, n, 0], self.e_sem.at[0, h, n], self.e_sem.at[1, h, n], self.p.far)

    def take(self, h, xres, w_post, act, w_pre):
        for n in PAIR:
            self.e_copy(h, n).wait()
        c = self.p.c

        def body(xb, _):
            for r in GROUPS:
                ys = [(self.es[h, n, xb, r, :].astype(F32) + self.er[h, n, xb, r, :].astype(F32)).astype(BF).astype(F32) for n in PAIR]
                inv = lax.rsqrt(sum(jnp.sum(y * y, axis=-1, keepdims=True) for y in ys) * (1.0 / D) + NORM_EPS)
                news = []
                for n in PAIR:
                    cols = slice(n * HALF, (n + 1) * HALF)
                    new = (xres[h, xb, r, cols].astype(F32) + ys[n] * inv * w_post[:, cols]).astype(BF)
                    xres[h, xb, r, cols] = new
                    news.append(new.astype(F32))
                inv = lax.rsqrt(sum(jnp.sum(v * v, axis=-1, keepdims=True) for v in news) * (1.0 / D) + NORM_EPS)
                for n in PAIR:
                    cols = slice(n * HALF, (n + 1) * HALF)
                    act[h, xb, c, r, cols] = (news[n] * inv * w_pre[:, cols]).astype(BF)
            return 0
        lax.fori_loop(0, 2, body, 0)

    def take_final(self, h, xres, w_post, out):
        for n in PAIR:
            self.f_copy(h, n).wait()
        x = self.p.x

        for r in GROUPS:
            ys = [(self.es[h, n, x, r, :].astype(F32) + self.er[h, n, 0, r, :].astype(F32)).astype(BF).astype(F32) for n in PAIR]
            inv = lax.rsqrt(sum(jnp.sum(y * y, axis=-1, keepdims=True) for y in ys) * (1.0 / D) + NORM_EPS)
            for n in PAIR:
                cols = slice(n * HALF, (n + 1) * HALF)
                out[h, r, cols] = (xres[h, x, r, cols].astype(F32) + ys[n] * inv * w_post[:, cols]).astype(BF)


class Shared:
    def __init__(self, peers, act, sem):
        self.p, self.act, self.sem = peers, act, sem

    def copy(self, h):
        view = self.act.at[h, :, self.p.c]
        return remote(view, view, self.sem.at[0, h], self.sem.at[1, h], self.p.mate)


def load(src, dst, sem):
    copy = pltpu.make_async_copy(src, dst, sem)
    copy.start()
    return copy


def gate_up(act, h, wg, wu, hid, between=None):
    def body(n, _):
        if between is not None:
            pl.when(n == 1)(between)
        g = act[h].reshape(TOK, D)
        gate = dot(g, wg[n])
        up = dot(g, wu[n])
        hid[:, pl.ds(pl.multiple_of(n * HALF, HALF), HALF)] = (jax.nn.gelu(gate, approximate=True) * up).astype(BF)
        return 0
    lax.fori_loop(0, 2, body, 0)


def down(hid, wd, n):
    return dot(hid[...], wd[n])


def layers_kernel(start, invf_in, norms_in, x_in, kl, vl, kg, vg, wq, wk, wv, wo, wg, wu, wd,
                  out_ref, k0_out, v0_out, k1_out, v1_out,
                  act, xres, kc, vc, qs, ks, vs, obuf, hid, pbuf, ds, dr, es, er, wgb, wub, wdb, wob, cosb, sinb, pa, pb, acc, tot, invf, norms,
                  ag_sem, d_sem, e_sem, g_sem, w_sem, o_sem, t_sem):
    p = Peers()
    copy_in = pltpu.make_async_copy
    qkv_loads = [[copy_in(w.at[l], buf.at[0, :, pl.ds(at, n)], w_sem.at[i]) for i, (w, at, n) in enumerate(((wq, 0, 512), (wk, 512, 256), (wv, 768, 256)))]
                 for l, buf in enumerate((wdb, wgb))]
    local_loads = [copy_in(kl, kc, w_sem.at[3]), copy_in(vl, vc, w_sem.at[4])]
    o_loads = [[copy_in(wo.at[l, :, pl.ds(n * HALF, HALF)], wob.at[n], w_sem.at[5 + n]) for n in PAIR] for l in PAIR]
    own = [copy_in(x_in.at[h], act.at[h, p.x, p.c], w_sem.at[7 + h]) for h in PAIR]
    mlp_loads = [[[copy_in(w.at[l, :, pl.ds(n * HALF, HALF)], buf.at[n], w_sem.at[9 + TWO * i + n]) for n in PAIR]
                  for i, (w, buf) in enumerate(((wg, wgb), (wu, wub), (wd, wdb)))] for l in PAIR]
    outs = [copy_in(src, dst, o_sem.at[i]) for i, (src, dst) in enumerate(((ks, k0_out), (vs, v0_out), (ks, k1_out), (vs, v1_out)))]

    def start_all(copies):
        for copy in copies:
            copy.start()

    def wait_all(copies):
        for copy in copies:
            copy.wait()

    params = [copy_in(invf_in, invf, o_sem.at[0]), copy_in(norms_in, norms, o_sem.at[1])]
    start_all(own + params)
    p.barrier()

    def ag_mate(h):
        view = act.at[h, p.x, p.c]
        return remote(view, view, ag_sem.at[0, 0, h], ag_sem.at[0, 1, h], p.mate)

    def ag_far(h):
        view = act.at[h, p.x, p.c]
        return remote(view, view, ag_sem.at[1, 0, h], ag_sem.at[1, 1, h], p.far)

    def ag_pass(h):
        view = act.at[h, 1 - p.x, p.c]
        return remote(view, view, ag_sem.at[2, 0, h], ag_sem.at[2, 1, h], p.mate)

    for h in PAIR:
        own[h].wait()
        ag_far(h).start()
        ag_mate(h).start()
    start_all(qkv_loads[0] + local_loads + o_loads[0])
    wait_all(params)

    for h in PAIR:
        pos = (lax.broadcasted_iota(jnp.int32, (TOK, 128), 0) + start[h]).astype(F32)
        angle = pos * invf[...]
        cosb[h] = jnp.cos(angle)
        sinb[h] = jnp.sin(angle)

    def scale(l, i):
        return 1.0 + norms[l, i:i + 1, :]

    def ag_arrive(h):
        ag_far(h).wait_recv()
        ag_pass(h).start()

    def ag_finish(h):
        ag_mate(h).wait_recv()
        ag_pass(h).wait()
        ag_mate(h).wait_send()
        ag_far(h).wait_send()
        xres[h] = act[h, :, p.c]
        norm_rows(act, h, scale(0, 0))

    def local_attention(h):
        q = qs[...]
        row = lax.broadcasted_iota(jnp.int32, (2 * TOK, 1), 0)
        i = jnp.where(row >= TOK, row - TOK, row)
        least = jnp.maximum(i + 1, WIN - start[h])
        acc = jnp.zeros((2 * TOK, HD), F32)
        total = jnp.zeros((2 * TOK, 1), F32)
        for b in PAIR:
            slot = lax.broadcasted_iota(jnp.int32, (1, 512), 1) + b * 512
            age = jnp.bitwise_and(slot - start[h], WIN - 1)
            wts = jnp.where(age >= least, soft_weights(dot_t(q, kc[h, b * 512:(b + 1) * 512, :])), 0.0)
            total += jnp.sum(wts, axis=-1, keepdims=True)
            acc += dot(wts.astype(BF), vc[h, b * 512:(b + 1) * 512, :])
        key = lax.broadcasted_iota(jnp.int32, (1, TOK), 1)
        wts = jnp.where(key <= i, soft_weights(dot_t(q, ks[h])), 0.0)
        total += jnp.sum(wts, axis=-1, keepdims=True)
        acc += dot(wts.astype(BF), vs[h])
        o = (acc / total).astype(BF)
        obuf[:, :HD] = o[:TOK]
        obuf[:, HD:] = o[TOK:]

    def exchange(s, er_slot, final=None):
        return Exchange(p, pbuf, ds, dr, es, er.at[er_slot], d_sem.at[s], e_sem.at[s], final)

    ex = [exchange(0, 0), exchange(1, 1), exchange(2, 0), exchange(3, 1)]
    sh = Shared(p, act, g_sem.at[1])

    def project(h, buf, q_dst):
        proj = dot(act[h].reshape(TOK, D), buf)
        rope_into(proj, cosb[h], sinb[h], q_dst, ks.at[h])
        vs[h] = proj[:, 768:].astype(BF)

    def first_attention():
        ag_arrive(0)
        for h in PAIR:
            ag_finish(h)
            if h == 0:
                wait_all(qkv_loads[0] + local_loads + o_loads[0])
                start_all(mlp_loads[0][0] + mlp_loads[0][1])
            project(h, wdb[0, :, :1024], qs)
            local_attention(h)
            for n in PAIR:
                ex[0].give(h, n, dot(obuf[...], wob[n]))
            if h == 0:
                ag_arrive(1)
            for n in PAIR:
                ex[0].send(h, n)
        start_all(mlp_loads[0][2] + outs[:2])

    def mlp(l):
        before, after = exchange(2 * l, 0), exchange(2 * l + 1, 1, l == 1)
        share = Shared(p, act, g_sem.at[2 * l])
        w_post, w_pre = scale(l, 1), scale(l, 2)
        before.take(0, xres, w_post, act, w_pre)
        share.copy(0).start()

        @pl.when(l == 1)
        def _():
            for n in PAIR:
                before.send(1, n)

        wait_all(mlp_loads[0][0] + mlp_loads[0][1])
        share.copy(0).wait()
        gate_up(act, 0, wgb, wub, hid)
        wait_all(mlp_loads[0][2])
        after.give(0, 0, down(hid, wdb, 0))
        before.take(1, xres, w_post, act, w_pre)
        share.copy(1).start()
        after.send(0, 0)
        after.give(0, 1, down(hid, wdb, 1))
        share.copy(1).wait()
        gate_up(act, 1, wgb, wub, hid, lambda: after.send(0, 1))
        for n in PAIR:
            after.give(1, n, down(hid, wdb, n))
        after.send(1, 0)

    def ring(a, g):
        s = lax.rem(g, 10)
        return wdb.at[s // 5, pl.ds(a * TILE, TILE), pl.ds(pl.multiple_of(lax.rem(s, 5) * HD, HD), HD)]

    def tile_in(a, g):
        src = (kg, vg)[a].at[g // NT, pl.ds(pl.multiple_of(lax.rem(g, NT) * TILE, TILE), TILE)]
        return pltpu.make_async_copy(src, ring(a, g), t_sem.at[a, g])

    def fetch(g):
        for a in PAIR:
            tile_in(a, g).wait()

        @pl.when(g + AHEAD < TWO * NT)
        def _():
            for a in PAIR:
                tile_in(a, g + AHEAD).start()

    row = lax.broadcasted_iota(jnp.int32, (2 * TOK, 1), 0)
    qi = jnp.where(row >= TOK, row - TOK, row)

    def global_attention(h):
        acc[...] = jnp.zeros_like(acc)
        tot[...] = jnp.zeros_like(tot)
        pb[...] = jnp.zeros_like(pb)
        base = h * NT

        def weigh(t, dst):
            keys = ring(0, base + t)
            for b in range(TILE // 256):
                scores = dot_t(qs[...], keys[b * 256:(b + 1) * 256, :])
                slot = lax.broadcasted_iota(jnp.int32, (1, 256), 1) + (t * TILE + b * 256)
                off = jnp.where(slot < start[h], S_OFF, HIDE)
                wts = jnp.exp2(jnp.tanh(scores * S_IN) * S_OUT - off)
                tot[...] += wts[:, :128] + wts[:, 128:]
                dst[:, b * 256:(b + 1) * 256] = wts.astype(BF)

        def four_tiles(i, _):
            t = 4 * i
            for j in range(4):
                fetch(base + t + j)
            part = dot(pb[...], ring(1, base + jnp.maximum(t - 1, 0))[...])
            for j, (dst, src) in enumerate(((pa, pa), (pb, pb), (pa, pa), (pb, None))):
                weigh(t + j, dst)
                if src is not None:
                    part += dot(src[...], ring(1, base + t + j)[...])
            acc[...] += part
            return 0

        lax.fori_loop(0, NT // 4, four_tiles, 0)
        before = dot(pb[...], ring(1, base + NT - 1)[...])
        wts = jnp.where(lax.broadcasted_iota(jnp.int32, (1, TOK), 1) <= qi, soft_weights(dot_t(qs[...], ks[h])), 0.0)
        total = jnp.sum(tot[...], axis=-1, keepdims=True) + jnp.sum(wts, axis=-1, keepdims=True)
        o = ((acc[...] + before + dot(wts.astype(BF), vs[h])) / total).astype(BF)
        obuf[:, :HD] = o[:TOK]
        obuf[:, HD:] = o[TOK:]

    def second_attention():
        start_all(qkv_loads[1])
        for g in range(AHEAD):
            for a in PAIR:
                tile_in(a, g).start()
        start_all(o_loads[1] + mlp_loads[1][1])
        ex[1].take(0, xres, scale(0, 3), act, scale(1, 0))
        sh.copy(0).start()
        ex[1].send(1, 1)
        wait_all(outs[:2] + qkv_loads[1])
        sh.copy(0).wait()
        project(0, wgb[0, :, :1024], qs)
        global_attention(0)
        ex[1].take(1, xres, scale(0, 3), act, scale(1, 0))
        sh.copy(1).start()
        wait_all(o_loads[1])
        for n in PAIR:
            ex[2].give(0, n, dot(obuf[...], wob[n]))
        ex[2].send(0, 0)
        sh.copy(1).wait()
        project(1, wgb[0, :, :1024], qs)
        ex[2].send(0, 1)
        start_all(mlp_loads[1][0])
        global_attention(1)
        for n in PAIR:
            ex[2].give(1, n, dot(obuf[...], wob[n]))
        start_all(outs[2:] + mlp_loads[1][2])

    def layer(l, _):
        pl.when(l == 0)(first_attention)
        pl.when(l == 1)(second_attention)
        mlp(l)
        return 0

    lax.fori_loop(0, 2, layer, 0)
    last = exchange(3, 1, True)
    last.take_final(0, xres, scale(1, 3), out_ref)
    last.send(1, 1)
    last.take_final(1, xres, scale(1, 3), out_ref)
    wait_all(outs[2:])


def shifted(ref, off, n):
    base = pl.multiple_of((off // 8) * 8, 8)
    rows = ref[pl.ds(base, n + 8), :]
    return pltpu.roll(rows, lax.rem(n + 8 - (off - base), n + 8), 0)[:n]


def cache_kernel(start, k_new, v_new, k0_new, v0_new, x_in, kl, vl, kg, vg,
                 x_out, kl_out, vl_out, kg_out, vg_out,
                 kb, vb, lbuf, ext, xbuf, fresh_rows, in_sem, out_sem, l_sem, f_sem):
    caches = ((kg, kb, kg_out, k_new), (vg, vb, vg_out, v_new))
    last = pl.ds(PAST, TOK)

    def tile(t):
        return pl.ds(pl.multiple_of(t * TILE, TILE), TILE)

    def rows_in(a, h, t, at):
        return pltpu.make_async_copy(caches[a][0].at[h, at], caches[a][1].at[h, at], in_sem.at[a, h, t])

    def rows_out(a, h, t, at):
        return pltpu.make_async_copy(caches[a][1].at[h, at], caches[a][2].at[h, at], out_sem.at[a, h, t])

    def each(h, body):
        lax.fori_loop(0, NT, lambda t, _: (body(h, t, tile(t)), 0)[1], 0)
        body(h, NT, last)

    def begin(h, t, at):
        for a in PAIR:
            rows_in(a, h, t, at).start()

    local = ((kl, k0_new, kl_out), (vl, v0_new, vl_out))
    for a in PAIR:
        pltpu.make_async_copy(local[a][0], lbuf.at[a], l_sem.at[a]).start()
    fresh_loads = [load(src, fresh_rows.at[i], f_sem.at[i]) for i, src in enumerate((k0_new, v0_new, k_new, v_new))]
    x_load = load(x_in, xbuf, l_sem.at[2])
    for h in PAIR:
        each(h, begin)

    def local_rows(a, h):
        fresh = fresh_rows[a, h].astype(F32)
        ext[0:TOK] = fresh
        ext[WIN:WIN + TOK] = fresh
        off = jnp.bitwise_and(-start[h], WIN - 1)

        def slots(b, _):
            lead = jnp.bitwise_and(b * 128 + off, WIN - 1)

            @pl.when((lead < TOK) | (lead > WIN - 128))
            def _():
                rows = shifted(ext, off + b * 128, 128)
                age = jnp.bitwise_and(lax.broadcasted_iota(jnp.int32, (128, 1), 0) + lead, WIN - 1)
                at = pl.ds(pl.multiple_of(b * 128, 128), 128)
                lbuf[a, h, at, :] = jnp.where(age < TOK, rows, lbuf[a, h, at, :].astype(F32)).astype(BF)

            return 0

        lax.fori_loop(0, WIN // 128, slots, 0)

    for copy in fresh_loads:
        copy.wait()
    for a in PAIR:
        pltpu.make_async_copy(local[a][0], lbuf.at[a], l_sem.at[a]).wait()
        for h in PAIR:
            local_rows(a, h)
        pltpu.make_async_copy(lbuf.at[a], local[a][2], l_sem.at[a]).start()
    x_load.wait()
    x_done = load(xbuf, x_out, l_sem.at[2])

    for h in PAIR:
        first = pl.multiple_of(jnp.minimum((start[h] // 16) * 16, CACHE - WROWS), 16)
        shift = first - start[h]

        def touched(t):
            return (t == first // TILE) | (t == (first + (WROWS - 1)) // TILE)

        def move(h, t, at):
            for a in PAIR:
                rows_in(a, h, t, at).wait()

            @pl.when(jnp.logical_not(touched(t)))
            def _():
                for a in PAIR:
                    rows_out(a, h, t, at).start()

        def move_touched(h, t, at):
            @pl.when(touched(t))
            def _():
                for a in PAIR:
                    rows_out(a, h, t, at).start()

        each(h, move)
        for a in PAIR:
            ext[16:16 + TOK] = fresh_rows[TWO + a, h].astype(F32)
            rows = shifted(ext, shift + 16, WROWS)
            idx = lax.broadcasted_iota(jnp.int32, (WROWS, 1), 0) + shift
            at = pl.ds(first, WROWS)
            buf = caches[a][1]
            buf[h, at, :] = jnp.where((idx >= 0) & (idx < TOK), rows, buf[h, at, :].astype(F32)).astype(BF)
        each(h, move_touched)

    def drain(h, t, at):
        for a in PAIR:
            rows_out(a, h, t, at).wait()

    for h in PAIR:
        each(h, drain)
    for a in PAIR:
        pltpu.make_async_copy(lbuf.at[a], local[a][2], l_sem.at[a]).wait()
    x_done.wait()


ANY = pl.BlockSpec(memory_space=pl.ANY)
VM = pl.BlockSpec(memory_space=pltpu.VMEM)
SM = pl.BlockSpec(memory_space=pltpu.SMEM)
DMA = pltpu.SemaphoreType.DMA


def vmem(*shape, dtype=BF):
    return pltpu.VMEM(shape, dtype)


def sds(*shape, dtype=BF):
    return jax.ShapeDtypeStruct(shape, dtype)


def run_layers(start, invf, norms, x, kl, vl, kg, vg, *weights):
    rows = sds(TWO, TOK, HD)
    pieces = vmem(TWO, TWO, TWO, BLK, HALF)
    return pl.pallas_call(
        layers_kernel,
        name="layers",
        out_shape=(sds(TWO, BLK, D), rows, rows, rows, rows),
        in_specs=[SM] + [ANY] * 14,
        out_specs=(VM, ANY, ANY, ANY, ANY),
        scratch_shapes=[
            vmem(TWO, TWO, TWO, BLK, D), vmem(TWO, TWO, BLK, D), vmem(TWO, WIN, HD), vmem(TWO, WIN, HD),
            vmem(TWO * TOK, HD), vmem(TWO, TOK, HD), vmem(TWO, TOK, HD),
            vmem(TOK, 512), vmem(TOK, D), vmem(TWO, TWO, TWO, BLK, HALF, dtype=F32),
            pieces, pieces, pieces, vmem(TWO, TWO, TWO, TWO, BLK, HALF),
            vmem(TWO, D, HALF), vmem(TWO, D, HALF), vmem(TWO, D, HALF), vmem(TWO, 512, HALF),
            vmem(TWO, TOK, 128, dtype=F32), vmem(TWO, TOK, 128, dtype=F32),
            vmem(TWO * TOK, TILE), vmem(TWO * TOK, TILE), vmem(TWO * TOK, HD, dtype=F32), vmem(TWO * TOK, 128, dtype=F32),
            vmem(1, 128, dtype=F32), vmem(TWO, 4, D, dtype=F32),
            DMA((3, TWO, TWO)), DMA((4, TWO, TWO, TWO)), DMA((4, TWO, TWO, TWO)), DMA((3, TWO, TWO)), DMA((15,)), DMA((4,)),
            DMA((TWO, TWO * NT)),
        ],
        compiler_params=pltpu.CompilerParams(collective_id=0, has_side_effects=True, vmem_limit_bytes=VMEM_LIMIT),
    )(start, invf, norms, x, kl, vl, kg, vg, *weights)


def run_caches(start, k_new, v_new, k0_new, v0_new, x, kl, vl, kg, vg):
    rows = vmem(TWO, CACHE, HD)
    return pl.pallas_call(
        cache_kernel,
        name="caches",
        out_shape=(sds(TWO, BLK, D), sds(TWO, WIN, HD), sds(TWO, WIN, HD), sds(TWO, CACHE, HD), sds(TWO, CACHE, HD)),
        in_specs=[SM] + [ANY] * 9,
        out_specs=(ANY,) * 5,
        scratch_shapes=[
            rows, rows, vmem(TWO, TWO, WIN, HD), vmem(TWO * WIN + 8, HD, dtype=F32), vmem(TWO, BLK, D), vmem(4, TWO, TOK, HD),
            DMA((TWO, TWO, NT + 1)), DMA((TWO, TWO, NT + 1)), DMA((3,)), DMA((4,)),
        ],
        compiler_params=pltpu.CompilerParams(has_side_effects=True, vmem_limit_bytes=VMEM_LIMIT),
    )(start, k_new, v_new, k0_new, v0_new, x, kl, vl, kg, vg)


def solution(mesh):
    act_spec = P('dp', 'tp', None)
    cache_spec = P('dp', None, 'tp', None)
    col_spec = P(None, None, 'tp')
    row_spec = P(None, 'tp', None)
    arg_specs = (act_spec, P('dp'), cache_spec, cache_spec, cache_spec, cache_spec, P(), col_spec, col_spec, col_spec, row_spec, col_spec, col_spec, row_spec)
    result_specs = (act_spec, cache_spec, cache_spec, cache_spec, cache_spec)
    inv_freq = np.power(np.float64(ROPE_BASE), np.arange(HD // 2) * (-2.0 / HD)).astype(np.float32)[None, :]

    def device_step(x, start, k_local, v_local, k_global, v_global, norms, w_q, w_k, w_v, w_o, w_gate, w_up, w_down):
        def flat(cache):
            return cache.reshape(cache.shape[0], cache.shape[1], cache.shape[3])

        kl, vl, kg, vg = flat(k_local), flat(v_local), flat(k_global), flat(v_global)
        invf = jnp.asarray(inv_freq)
        out, k0, v0, k1, v1 = run_layers(start, invf, norms, x, kl, vl, kg, vg, w_q, w_k, w_v, w_o, w_gate, w_up, w_down)
        out, kl_new, vl_new, kg_new, vg_new = run_caches(start, k1, v1, k0, v0, out, kl, vl, kg, vg)
        return (out, kl_new.reshape(k_local.shape), vl_new.reshape(v_local.shape), kg_new.reshape(k_global.shape), vg_new.reshape(v_global.shape))

    return jax.shard_map(device_step, mesh=mesh, in_specs=arg_specs, out_specs=result_specs, check_vma=False)
```

```python
import functools

import jax
import jax.numpy as jnp
import numpy as np
from jax import lax
from jax.experimental import pallas as pl
from jax.experimental.pallas import tpu as pltpu
from jax.sharding import PartitionSpec as P

BF = jnp.bfloat16
F32 = jnp.float32
MESH = pl.DeviceIdType.MESH
NORM_EPS = 1e-6
ROPE_BASE = 10000.0
LOG2E = 1.4426950408889634
S_IN = 1.0 / (50.0 * 16.0)
S_OUT = 50.0 * LOG2E
S_OFF = 36.0 * LOG2E

D = 2560
HALF = 1280
TOK = 192
BLK = 48
HD = 256
WIN = 1024
VMEM_LIMIT = 67000000
TWO = 2
PAIR = range(TWO)
GROUPS = tuple(slice(i, i + 16) for i in range(0, BLK, 16))


TILE = 1024
PAST = 12288
CACHE = PAST + TOK
NT = PAST // TILE
WROWS = TOK + 16
AHEAD = 5
HIDE = 1e6


def dot(a, b):
    return jnp.dot(a, b, preferred_element_type=F32)


def dot_t(a, b):
    return lax.dot_general(a, b, (((1,), (1,)), ((), ())), preferred_element_type=F32)


def soft_weights(scores):
    return jnp.exp2(jnp.tanh(scores * S_IN) * S_OUT - S_OFF)


def rope_into(proj, cos, sin, q_dst, k_dst):
    for head, (ref, row) in enumerate(((q_dst, 0), (q_dst, TOK), (k_dst, 0))):
        lead = proj[:, head * HD:head * HD + 128]
        tail = proj[:, head * HD + 128:(head + 1) * HD]
        ref[row:row + TOK, :128] = (lead * cos - tail * sin).astype(BF)
        ref[row:row + TOK, 128:] = (tail * cos + lead * sin).astype(BF)


class Peers:
    def __init__(self):
        dp = lax.axis_index("dp")
        tp = lax.axis_index("tp")
        self.x = tp // 2
        self.c = lax.rem(tp, 2)
        self.mate = (dp, tp + 1 - 2 * self.c)
        self.far = (dp, lax.rem(tp + 2, 4))

    def barrier(self):
        sem = pltpu.get_barrier_semaphore()
        for peer in (self.mate, self.far):
            pl.semaphore_signal(sem, inc=1, device_id=peer, device_id_type=MESH)
        pl.semaphore_wait(sem, 2)


def remote(src, dst, send, recv, peer):
    return pltpu.make_async_remote_copy(src_ref=src, dst_ref=dst, send_sem=send, recv_sem=recv, device_id=peer, device_id_type=MESH)


def norm_rows(act, h, w):
    def body(i, _):
        for r in GROUPS:
            rows = act[h, i // 2, i % 2, r, :].astype(F32)
            inv = lax.rsqrt(jnp.sum(rows * rows, axis=-1, keepdims=True) * (1.0 / D) + NORM_EPS)
            act[h, i // 2, i % 2, r, :] = (rows * inv * w).astype(BF)
        return 0
    lax.fori_loop(0, 4, body, 0)


class Exchange:
    def __init__(self, peers, pbuf, ds, dr, es, er, d_sem, e_sem, final=None):
        self.p, self.pbuf, self.ds, self.dr, self.es, self.er = peers, pbuf, ds, dr, es, er
        self.d_sem, self.e_sem, self.final = d_sem, e_sem, final

    def d_copy(self, h, n):
        return remote(self.ds.at[h, n], self.dr.at[h, n], self.d_sem.at[0, h, n], self.d_sem.at[1, h, n], self.p.mate)

    def e_copy(self, h, n):
        return remote(self.es.at[h, n], self.er.at[h, n], self.e_sem.at[0, h, n], self.e_sem.at[1, h, n], self.p.far)

    def give(self, h, n, part):
        self.pbuf[n] = part.reshape(2, 2, BLK, HALF)
        self.ds[h, n] = self.pbuf[n, :, 1 - self.p.c].astype(BF)
        self.d_copy(h, n).start()

    def send(self, h, n):
        copy = self.d_copy(h, n)
        copy.wait_recv()
        self.es[h, n] = (self.pbuf[n, :, self.p.c] + self.dr[h, n].astype(F32)).astype(BF)
        if self.final is None:
            self.e_copy(h, n).start()
        else:
            pl.when(self.final)(lambda: self.f_copy(h, n).start())
            pl.when(jnp.logical_not(self.final))(lambda: self.e_copy(h, n).start())
        copy.wait_send()

    def f_copy(self, h, n):
        return remote(self.es.at[h, n, 1 - self.p.x], self.er.at[h, n, 0], self.e_sem.at[0, h, n], self.e_sem.at[1, h, n], self.p.far)

    def take(self, h, xres, w_post, act, w_pre):
        for n in PAIR:
            self.e_copy(h, n).wait()
        c = self.p.c

        def body(xb, _):
            for r in GROUPS:
                ys = [(self.es[h, n, xb, r, :].astype(F32) + self.er[h, n, xb, r, :].astype(F32)).astype(BF).astype(F32) for n in PAIR]
                inv = lax.rsqrt(sum(jnp.sum(y * y, axis=-1, keepdims=True) for y in ys) * (1.0 / D) + NORM_EPS)
                news = []
                for n in PAIR:
                    cols = slice(n * HALF, (n + 1) * HALF)
                    new = (xres[h, xb, r, cols].astype(F32) + ys[n] * inv * w_post[:, cols]).astype(BF)
                    xres[h, xb, r, cols] = new
                    news.append(new.astype(F32))
                inv = lax.rsqrt(sum(jnp.sum(v * v, axis=-1, keepdims=True) for v in news) * (1.0 / D) + NORM_EPS)
                for n in PAIR:
                    cols = slice(n * HALF, (n + 1) * HALF)
                    act[h, xb, c, r, cols] = (news[n] * inv * w_pre[:, cols]).astype(BF)
            return 0
        lax.fori_loop(0, 2, body, 0)

    def take_final(self, h, xres, w_post, out):
        for n in PAIR:
            self.f_copy(h, n).wait()
        x = self.p.x

        for r in GROUPS:
            ys = [(self.es[h, n, x, r, :].astype(F32) + self.er[h, n, 0, r, :].astype(F32)).astype(BF).astype(F32) for n in PAIR]
            inv = lax.rsqrt(sum(jnp.sum(y * y, axis=-1, keepdims=True) for y in ys) * (1.0 / D) + NORM_EPS)
            for n in PAIR:
                cols = slice(n * HALF, (n + 1) * HALF)
                out[h, r, cols] = (xres[h, x, r, cols].astype(F32) + ys[n] * inv * w_post[:, cols]).astype(BF)


class Shared:
    def __init__(self, peers, act, sem):
        self.p, self.act, self.sem = peers, act, sem

    def copy(self, h):
        view = self.act.at[h, :, self.p.c]
        return remote(view, view, self.sem.at[0, h], self.sem.at[1, h], self.p.mate)


def load(src, dst, sem):
    copy = pltpu.make_async_copy(src, dst, sem)
    copy.start()
    return copy


def gate_up(act, h, wg, wu, hid, between=None):
    def body(n, _):
        if between is not None:
            pl.when(n == 1)(between)
        g = act[h].reshape(TOK, D)
        gate = dot(g, wg[n])
        up = dot(g, wu[n])
        hid[:, pl.ds(pl.multiple_of(n * HALF, HALF), HALF)] = (jax.nn.gelu(gate, approximate=True) * up).astype(BF)
        return 0
    lax.fori_loop(0, 2, body, 0)


def down(hid, wd, n):
    return dot(hid[...], wd[n])


def layers_kernel(start, invf_in, norms_in, x_in, kl, vl, kg, vg, wq, wk, wv, wo, wg, wu, wd,
                  out_ref, k0_out, v0_out, k1_out, v1_out,
                  act, xres, kc, vc, qs, ks, vs, obuf, hid, pbuf, ds, dr, es, er, wgb, wub, wdb, wob, cosb, sinb, pa, pb, acc, tot, invf, norms,
                  ag_sem, d_sem, e_sem, g_sem, w_sem, o_sem, t_sem):
    p = Peers()
    copy_in = pltpu.make_async_copy
    qkv_loads = [[copy_in(w.at[l], buf.at[0, :, pl.ds(at, n)], w_sem.at[i]) for i, (w, at, n) in enumerate(((wq, 0, 512), (wk, 512, 256), (wv, 768, 256)))]
                 for l, buf in enumerate((wdb, wgb))]
    local_loads = [copy_in(kl, kc, w_sem.at[3]), copy_in(vl, vc, w_sem.at[4])]
    o_loads = [[copy_in(wo.at[l, :, pl.ds(n * HALF, HALF)], wob.at[n], w_sem.at[5 + n]) for n in PAIR] for l in PAIR]
    own = [copy_in(x_in.at[h], act.at[h, p.x, p.c], w_sem.at[7 + h]) for h in PAIR]
    mlp_loads = [[[copy_in(w.at[l, :, pl.ds(n * HALF, HALF)], buf.at[n], w_sem.at[9 + TWO * i + n]) for n in PAIR]
                  for i, (w, buf) in enumerate(((wg, wgb), (wu, wub), (wd, wdb)))] for l in PAIR]
    outs = [copy_in(src, dst, o_sem.at[i]) for i, (src, dst) in enumerate(((ks, k0_out), (vs, v0_out), (ks, k1_out), (vs, v1_out)))]

    def start_all(copies):
        for copy in copies:
            copy.start()

    def wait_all(copies):
        for copy in copies:
            copy.wait()

    params = [copy_in(invf_in, invf, o_sem.at[0]), copy_in(norms_in, norms, o_sem.at[1])]
    start_all(own + params)
    p.barrier()

    def ag_mate(h):
        view = act.at[h, p.x, p.c]
        return remote(view, view, ag_sem.at[0, 0, h], ag_sem.at[0, 1, h], p.mate)

    def ag_far(h):
        view = act.at[h, p.x, p.c]
        return remote(view, view, ag_sem.at[1, 0, h], ag_sem.at[1, 1, h], p.far)

    def ag_pass(h):
        view = act.at[h, 1 - p.x, p.c]
        return remote(view, view, ag_sem.at[2, 0, h], ag_sem.at[2, 1, h], p.mate)

    for h in PAIR:
        own[h].wait()
        ag_far(h).start()
        ag_mate(h).start()
    start_all(qkv_loads[0] + local_loads + o_loads[0])
    wait_all(params)

    for h in PAIR:
        pos = (lax.broadcasted_iota(jnp.int32, (TOK, 128), 0) + start[h]).astype(F32)
        angle = pos * invf[...]
        cosb[h] = jnp.cos(angle)
        sinb[h] = jnp.sin(angle)

    def scale(l, i):
        return 1.0 + norms[l, i:i + 1, :]

    def ag_arrive(h):
        ag_far(h).wait_recv()
        ag_pass(h).start()

    def ag_finish(h):
        ag_mate(h).wait_recv()
        ag_pass(h).wait()
        ag_mate(h).wait_send()
        ag_far(h).wait_send()
        xres[h] = act[h, :, p.c]
        norm_rows(act, h, scale(0, 0))

    def local_attention(h):
        q = qs[...]
        row = lax.broadcasted_iota(jnp.int32, (2 * TOK, 1), 0)
        i = jnp.where(row >= TOK, row - TOK, row)
        least = jnp.maximum(i + 1, WIN - start[h])
        acc = jnp.zeros((2 * TOK, HD), F32)
        total = jnp.zeros((2 * TOK, 1), F32)
        for b in PAIR:
            slot = lax.broadcasted_iota(jnp.int32, (1, 512), 1) + b * 512
            age = jnp.bitwise_and(slot - start[h], WIN - 1)
            wts = jnp.where(age >= least, soft_weights(dot_t(q, kc[h, b * 512:(b + 1) * 512, :])), 0.0)
            total += jnp.sum(wts, axis=-1, keepdims=True)
            acc += dot(wts.astype(BF), vc[h, b * 512:(b + 1) * 512, :])
        key = lax.broadcasted_iota(jnp.int32, (1, TOK), 1)
        wts = jnp.where(key <= i, soft_weights(dot_t(q, ks[h])), 0.0)
        total += jnp.sum(wts, axis=-1, keepdims=True)
        acc += dot(wts.astype(BF), vs[h])
        o = (acc / total).astype(BF)
        obuf[:, :HD] = o[:TOK]
        obuf[:, HD:] = o[TOK:]

    def exchange(s, er_slot, final=None):
        return Exchange(p, pbuf, ds, dr, es, er.at[er_slot], d_sem.at[s], e_sem.at[s], final)

    ex = [exchange(0, 0), exchange(1, 1), exchange(2, 0), exchange(3, 1)]
    sh = Shared(p, act, g_sem.at[1])

    def project(h, buf, q_dst):
        proj = dot(act[h].reshape(TOK, D), buf)
        rope_into(proj, cosb[h], sinb[h], q_dst, ks.at[h])
        vs[h] = proj[:, 768:].astype(BF)

    def first_attention():
        ag_arrive(0)
        for h in PAIR:
            ag_finish(h)
            if h == 0:
                wait_all(qkv_loads[0] + local_loads + o_loads[0])
                start_all(mlp_loads[0][0] + mlp_loads[0][1])
            project(h, wdb[0, :, :1024], qs)
            local_attention(h)
            for n in PAIR:
                ex[0].give(h, n, dot(obuf[...], wob[n]))
            if h == 0:
                ag_arrive(1)
            for n in PAIR:
                ex[0].send(h, n)
        start_all(mlp_loads[0][2] + outs[:2])

    def mlp(l):
        before, after = exchange(2 * l, 0), exchange(2 * l + 1, 1, l == 1)
        share = Shared(p, act, g_sem.at[2 * l])
        w_post, w_pre = scale(l, 1), scale(l, 2)
        before.take(0, xres, w_post, act, w_pre)
        share.copy(0).start()

        @pl.when(l == 1)
        def _():
            for n in PAIR:
                before.send(1, n)

        wait_all(mlp_loads[0][0] + mlp_loads[0][1])
        share.copy(0).wait()
        gate_up(act, 0, wgb, wub, hid)
        wait_all(mlp_loads[0][2])
        after.give(0, 0, down(hid, wdb, 0))
        before.take(1, xres, w_post, act, w_pre)
        share.copy(1).start()
        after.send(0, 0)
        after.give(0, 1, down(hid, wdb, 1))
        share.copy(1).wait()
        gate_up(act, 1, wgb, wub, hid, lambda: after.send(0, 1))

        @pl.when(l == 0)
        def _():
            start_all(qkv_loads[1] + mlp_loads[1][1])

        for n in PAIR:
            after.give(1, n, down(hid, wdb, n))
        after.send(1, 0)

    def ring(a, g):
        s = lax.rem(g, 10)
        return wdb.at[s // 5, pl.ds(a * TILE, TILE), pl.ds(pl.multiple_of(lax.rem(s, 5) * HD, HD), HD)]

    def tile_in(a, g):
        src = (kg, vg)[a].at[g // NT, pl.ds(pl.multiple_of(lax.rem(g, NT) * TILE, TILE), TILE)]
        return pltpu.make_async_copy(src, ring(a, g), t_sem.at[a, g])

    def fetch(g):
        for a in PAIR:
            tile_in(a, g).wait()

        @pl.when(g + AHEAD < TWO * NT)
        def _():
            for a in PAIR:
                tile_in(a, g + AHEAD).start()

    row = lax.broadcasted_iota(jnp.int32, (2 * TOK, 1), 0)
    qi = jnp.where(row >= TOK, row - TOK, row)

    def global_attention(h):
        acc[...] = jnp.zeros_like(acc)
        tot[...] = jnp.zeros_like(tot)
        pb[...] = jnp.zeros_like(pb)
        base = h * NT

        def weigh(t, dst):
            keys = ring(0, base + t)
            for b in range(TILE // 256):
                scores = dot_t(qs[...], keys[b * 256:(b + 1) * 256, :])
                slot = lax.broadcasted_iota(jnp.int32, (1, 256), 1) + (t * TILE + b * 256)
                off = jnp.where(slot < start[h], S_OFF, HIDE)
                wts = jnp.exp2(jnp.tanh(scores * S_IN) * S_OUT - off)
                tot[...] += wts[:, :128] + wts[:, 128:]
                dst[:, b * 256:(b + 1) * 256] = wts.astype(BF)

        def four_tiles(i, _):
            t = 4 * i
            for j in range(4):
                fetch(base + t + j)
            part = dot(pb[...], ring(1, base + jnp.maximum(t - 1, 0))[...])
            for j, (dst, src) in enumerate(((pa, pa), (pb, pb), (pa, pa), (pb, None))):
                weigh(t + j, dst)
                if src is not None:
                    part += dot(src[...], ring(1, base + t + j)[...])
            acc[...] += part
            return 0

        lax.fori_loop(0, NT // 4, four_tiles, 0)
        before = dot(pb[...], ring(1, base + NT - 1)[...])
        wts = jnp.where(lax.broadcasted_iota(jnp.int32, (1, TOK), 1) <= qi, soft_weights(dot_t(qs[...], ks[h])), 0.0)
        total = jnp.sum(tot[...], axis=-1, keepdims=True) + jnp.sum(wts, axis=-1, keepdims=True)
        o = ((acc[...] + before + dot(wts.astype(BF), vs[h])) / total).astype(BF)
        obuf[:, :HD] = o[:TOK]
        obuf[:, HD:] = o[TOK:]

    def second_attention():
        for g in range(AHEAD):
            for a in PAIR:
                tile_in(a, g).start()
        start_all(o_loads[1])
        ex[1].take(0, xres, scale(0, 3), act, scale(1, 0))
        sh.copy(0).start()
        ex[1].send(1, 1)
        wait_all(outs[:2] + qkv_loads[1])
        sh.copy(0).wait()
        project(0, wgb[0, :, :1024], qs)
        global_attention(0)
        ex[1].take(1, xres, scale(0, 3), act, scale(1, 0))
        sh.copy(1).start()
        wait_all(o_loads[1])
        for n in PAIR:
            ex[2].give(0, n, dot(obuf[...], wob[n]))
        ex[2].send(0, 0)
        sh.copy(1).wait()
        project(1, wgb[0, :, :1024], qs)
        ex[2].send(0, 1)
        start_all(mlp_loads[1][0])
        global_attention(1)
        for n in PAIR:
            ex[2].give(1, n, dot(obuf[...], wob[n]))
        start_all(outs[2:] + mlp_loads[1][2])

    def layer(l, _):
        pl.when(l == 0)(first_attention)
        pl.when(l == 1)(second_attention)
        mlp(l)
        return 0

    lax.fori_loop(0, 2, layer, 0)
    last = exchange(3, 1, True)
    last.take_final(0, xres, scale(1, 3), out_ref)
    last.send(1, 1)
    last.take_final(1, xres, scale(1, 3), out_ref)
    wait_all(outs[2:])


def shifted(ref, off, n):
    base = pl.multiple_of((off // 8) * 8, 8)
    rows = ref[pl.ds(base, n + 8), :]
    return pltpu.roll(rows, lax.rem(n + 8 - (off - base), n + 8), 0)[:n]


def cache_kernel(start, k_new, v_new, k0_new, v0_new, x_in, kl, vl, kg, vg,
                 x_out, kl_out, vl_out, kg_out, vg_out,
                 kb, vb, lbuf, ext, xbuf, fresh_rows, in_sem, out_sem, l_sem, f_sem):
    caches = ((kg, kb, kg_out, k_new), (vg, vb, vg_out, v_new))
    last = pl.ds(PAST, TOK)

    def tile(t):
        return pl.ds(pl.multiple_of(t * TILE, TILE), TILE)

    def rows_in(a, h, t, at):
        return pltpu.make_async_copy(caches[a][0].at[h, at], caches[a][1].at[h, at], in_sem.at[a, h, t])

    def rows_out(a, h, t, at):
        return pltpu.make_async_copy(caches[a][1].at[h, at], caches[a][2].at[h, at], out_sem.at[a, h, t])

    def each(h, body):
        lax.fori_loop(0, NT, lambda t, _: (body(h, t, tile(t)), 0)[1], 0)
        body(h, NT, last)

    def begin(h, t, at):
        for a in PAIR:
            rows_in(a, h, t, at).start()

    local = ((kl, k0_new, kl_out), (vl, v0_new, vl_out))
    for a in PAIR:
        pltpu.make_async_copy(local[a][0], lbuf.at[a], l_sem.at[a]).start()
    fresh_loads = [load(src, fresh_rows.at[i], f_sem.at[i]) for i, src in enumerate((k0_new, v0_new, k_new, v_new))]
    x_load = load(x_in, xbuf, l_sem.at[2])
    for h in PAIR:
        each(h, begin)

    def local_rows(a, h):
        fresh = fresh_rows[a, h].astype(F32)
        ext[0:TOK] = fresh
        ext[WIN:WIN + TOK] = fresh
        off = jnp.bitwise_and(-start[h], WIN - 1)

        def slots(b, _):
            lead = jnp.bitwise_and(b * 128 + off, WIN - 1)

            @pl.when((lead < TOK) | (lead > WIN - 128))
            def _():
                rows = shifted(ext, off + b * 128, 128)
                age = jnp.bitwise_and(lax.broadcasted_iota(jnp.int32, (128, 1), 0) + lead, WIN - 1)
                at = pl.ds(pl.multiple_of(b * 128, 128), 128)
                lbuf[a, h, at, :] = jnp.where(age < TOK, rows, lbuf[a, h, at, :].astype(F32)).astype(BF)

            return 0

        lax.fori_loop(0, WIN // 128, slots, 0)

    for copy in fresh_loads:
        copy.wait()
    for a in PAIR:
        pltpu.make_async_copy(local[a][0], lbuf.at[a], l_sem.at[a]).wait()
        for h in PAIR:
            local_rows(a, h)
        pltpu.make_async_copy(lbuf.at[a], local[a][2], l_sem.at[a]).start()
    x_load.wait()
    x_done = load(xbuf, x_out, l_sem.at[2])

    for h in PAIR:
        first = pl.multiple_of(jnp.minimum((start[h] // 16) * 16, CACHE - WROWS), 16)
        shift = first - start[h]

        def touched(t):
            return (t == first // TILE) | (t == (first + (WROWS - 1)) // TILE)

        def move(h, t, at):
            for a in PAIR:
                rows_in(a, h, t, at).wait()

            @pl.when(jnp.logical_not(touched(t)))
            def _():
                for a in PAIR:
                    rows_out(a, h, t, at).start()

        def move_touched(h, t, at):
            @pl.when(touched(t))
            def _():
                for a in PAIR:
                    rows_out(a, h, t, at).start()

        each(h, move)
        for a in PAIR:
            ext[16:16 + TOK] = fresh_rows[TWO + a, h].astype(F32)
            rows = shifted(ext, shift + 16, WROWS)
            idx = lax.broadcasted_iota(jnp.int32, (WROWS, 1), 0) + shift
            at = pl.ds(first, WROWS)
            buf = caches[a][1]
            buf[h, at, :] = jnp.where((idx >= 0) & (idx < TOK), rows, buf[h, at, :].astype(F32)).astype(BF)
        each(h, move_touched)

    def drain(h, t, at):
        for a in PAIR:
            rows_out(a, h, t, at).wait()

    for h in PAIR:
        each(h, drain)
    for a in PAIR:
        pltpu.make_async_copy(lbuf.at[a], local[a][2], l_sem.at[a]).wait()
    x_done.wait()


ANY = pl.BlockSpec(memory_space=pl.ANY)
VM = pl.BlockSpec(memory_space=pltpu.VMEM)
SM = pl.BlockSpec(memory_space=pltpu.SMEM)
DMA = pltpu.SemaphoreType.DMA


def vmem(*shape, dtype=BF):
    return pltpu.VMEM(shape, dtype)


def sds(*shape, dtype=BF):
    return jax.ShapeDtypeStruct(shape, dtype)


def run_layers(start, invf, norms, x, kl, vl, kg, vg, *weights):
    rows = sds(TWO, TOK, HD)
    pieces = vmem(TWO, TWO, TWO, BLK, HALF)
    return pl.pallas_call(
        layers_kernel,
        name="layers",
        out_shape=(sds(TWO, BLK, D), rows, rows, rows, rows),
        in_specs=[SM] + [ANY] * 14,
        out_specs=(VM, ANY, ANY, ANY, ANY),
        scratch_shapes=[
            vmem(TWO, TWO, TWO, BLK, D), vmem(TWO, TWO, BLK, D), vmem(TWO, WIN, HD), vmem(TWO, WIN, HD),
            vmem(TWO * TOK, HD), vmem(TWO, TOK, HD), vmem(TWO, TOK, HD),
            vmem(TOK, 512), vmem(TOK, D), vmem(TWO, TWO, TWO, BLK, HALF, dtype=F32),
            pieces, pieces, pieces, vmem(TWO, TWO, TWO, TWO, BLK, HALF),
            vmem(TWO, D, HALF), vmem(TWO, D, HALF), vmem(TWO, D, HALF), vmem(TWO, 512, HALF),
            vmem(TWO, TOK, 128, dtype=F32), vmem(TWO, TOK, 128, dtype=F32),
            vmem(TWO * TOK, TILE), vmem(TWO * TOK, TILE), vmem(TWO * TOK, HD, dtype=F32), vmem(TWO * TOK, 128, dtype=F32),
            vmem(1, 128, dtype=F32), vmem(TWO, 4, D, dtype=F32),
            DMA((3, TWO, TWO)), DMA((4, TWO, TWO, TWO)), DMA((4, TWO, TWO, TWO)), DMA((3, TWO, TWO)), DMA((15,)), DMA((4,)),
            DMA((TWO, TWO * NT)),
        ],
        compiler_params=pltpu.CompilerParams(collective_id=0, has_side_effects=True, vmem_limit_bytes=VMEM_LIMIT),
    )(start, invf, norms, x, kl, vl, kg, vg, *weights)


def run_caches(start, k_new, v_new, k0_new, v0_new, x, kl, vl, kg, vg):
    rows = vmem(TWO, CACHE, HD)
    return pl.pallas_call(
        cache_kernel,
        name="caches",
        out_shape=(sds(TWO, BLK, D), sds(TWO, WIN, HD), sds(TWO, WIN, HD), sds(TWO, CACHE, HD), sds(TWO, CACHE, HD)),
        in_specs=[SM] + [ANY] * 9,
        out_specs=(ANY,) * 5,
        scratch_shapes=[
            rows, rows, vmem(TWO, TWO, WIN, HD), vmem(TWO * WIN + 8, HD, dtype=F32), vmem(TWO, BLK, D), vmem(4, TWO, TOK, HD),
            DMA((TWO, TWO, NT + 1)), DMA((TWO, TWO, NT + 1)), DMA((3,)), DMA((4,)),
        ],
        compiler_params=pltpu.CompilerParams(has_side_effects=True, vmem_limit_bytes=VMEM_LIMIT),
    )(start, k_new, v_new, k0_new, v0_new, x, kl, vl, kg, vg)


def solution(mesh):
    act_spec = P('dp', 'tp', None)
    cache_spec = P('dp', None, 'tp', None)
    col_spec = P(None, None, 'tp')
    row_spec = P(None, 'tp', None)
    arg_specs = (act_spec, P('dp'), cache_spec, cache_spec, cache_spec, cache_spec, P(), col_spec, col_spec, col_spec, row_spec, col_spec, col_spec, row_spec)
    result_specs = (act_spec, cache_spec, cache_spec, cache_spec, cache_spec)
    inv_freq = np.power(np.float64(ROPE_BASE), np.arange(HD // 2) * (-2.0 / HD)).astype(np.float32)[None, :]

    def device_step(x, start, k_local, v_local, k_global, v_global, norms, w_q, w_k, w_v, w_o, w_gate, w_up, w_down):
        def flat(cache):
            return cache.reshape(cache.shape[0], cache.shape[1], cache.shape[3])

        kl, vl, kg, vg = flat(k_local), flat(v_local), flat(k_global), flat(v_global)
        invf = jnp.asarray(inv_freq)
        out, k0, v0, k1, v1 = run_layers(start, invf, norms, x, kl, vl, kg, vg, w_q, w_k, w_v, w_o, w_gate, w_up, w_down)
        out, kl_new, vl_new, kg_new, vg_new = run_caches(start, k1, v1, k0, v0, out, kl, vl, kg, vg)
        return (out, kl_new.reshape(k_local.shape), vl_new.reshape(v_local.shape), kg_new.reshape(k_global.shape), vg_new.reshape(v_global.shape))

    return jax.shard_map(device_step, mesh=mesh, in_specs=arg_specs, out_specs=result_specs, check_vma=False)
```
